256 devices in a mesh: gx: 32 (over z, y), gy: 8 (over x, core).
Axes of the slice: x: 4, y: 4, z: 8, core: 2. Of those that a mesh axis runs over, the one named last changes fastest.
Arguments:
- spins: bfloat16 [16, 128, 512, 256], P(None, 'gx', 'gy'), may hold values from -1 to 1
- couplings: int32 [6, 128, 512, 256], P(None, 'gx', 'gy'), may hold values from -1 to 1, as said below
- betas: float32 [16], replicated, may hold values from 0.25 to 1.5
- metro_uniform: bfloat16 [2, 16, 128, 512, 256], P(None, None, 'gx', 'gy'), may hold values from 0 to 1
- swap_uniform: float32 [8], replicated, may hold values from 0.8 to 1
Outputs:
- spins_out: bfloat16 [16, 128, 512, 256], P(None, 'gx', 'gy')
- energies: float32 [16], replicated
The draws below stay inside these ranges and needn't reach their ends.
Inputs may be any that keep to these rules, and one draw needn't show every extreme that they name: Every entry is -1 or 1; couplings[3 + d] at a cell equals couplings[d] at the cell one step lower along lattice dimension d, with periodic wrap.
All inputs are finite; a program needn't handle non-finite values.
Results may differ from the reference program's by a relative error of at most 0.0085.
Values may be sent and summed in bfloat16 or wider, within the bound.
No kernel may reach another device: no remote copies, remote signals or barrier semaphores. Data moves between devices by JAX's collectives and lax.ppermute only.
A program may use at most 128 MiB of HBM per device.

```python
import jax
import jax.numpy as jnp
from jax import lax

R = 16
SWEEPS = 2
CX = 4
CY = 64
NZ = 256
NX = 128
NY = 512


def common_signs(key):
    pattern = 2 * jax.random.randint(jax.random.fold_in(key, 5), (NX, NY, NZ), 0, 2) - 1
    return pattern


def replica_flips(key):
    return 2 * jax.random.randint(jax.random.fold_in(key, 7), (R,), 0, 2) - 1


def draw_spins(key, part):
    shape = (R, NX, NY, NZ)
    pair_count = R // 2
    x_blocks = NX // CX
    y_blocks = NY // CY
    pattern = common_signs(key)
    flips = replica_flips(key)
    aligned = (flips[:, None, None, None] * pattern[None]).astype(jnp.float32)
    scattered = (2 * jax.random.randint(jax.random.fold_in(key, 8), shape, 0, 2) - 1).astype(jnp.float32)
    position = jnp.arange(NX, dtype=jnp.float32) / jnp.float32(NX - 1)
    ramp_line = 0.55 + 0.45 * position
    x_gain = jax.random.uniform(jax.random.fold_in(key, 12), (pair_count, x_blocks), jnp.float32, 0.35, 1.0)
    y_gain = jax.random.uniform(jax.random.fold_in(key, 13), (pair_count, y_blocks), jnp.float32, 0.7, 1.0)
    spread = jax.random.uniform(jax.random.fold_in(key, 6), shape, jnp.float32, 0.7, 1.0)
    order_frac = jax.random.uniform(jax.random.fold_in(key, 14), (pair_count, x_blocks), jnp.float32, 0.0, 1.0)
    x_cells = jnp.repeat(x_gain, CX, axis=1)
    y_cells = jnp.repeat(y_gain, CY, axis=1)
    order_cells = jnp.repeat(order_frac, CX, axis=1)
    leading = ramp_line[None, :, None] * x_cells[:, :, None] * y_cells[:, None, :]
    mirrored = leading[:, ::-1, ::-1]
    amplitude = jnp.stack([leading, mirrored], axis=1).reshape(R, NX, NY)
    lead_order = jnp.broadcast_to(order_cells[:, :, None], (pair_count, NX, NY))
    order_field = jnp.stack([lead_order, lead_order[:, ::-1, ::-1]], axis=1).reshape(R, NX, NY)
    choose = jax.random.uniform(jax.random.fold_in(key, 15), shape, jnp.float32, 0.0, 1.0) < order_field[..., None]
    sign_field = jnp.where(choose, aligned, scattered)
    return (sign_field * amplitude[..., None] * spread).astype(jnp.bfloat16)


def draw_couplings(key, part):
    shape = (2, NX, NY, NZ)
    pattern = common_signs(key)
    along_x = pattern * jnp.roll(pattern, -1, 0)
    others = 2 * jax.random.randint(jax.random.fold_in(key, 11), shape, 0, 2) - 1
    forward = jnp.concatenate([along_x[None], others], axis=0)
    backward = jnp.stack([jnp.roll(forward[0], 1, 0), jnp.roll(forward[1], 1, 1), jnp.roll(forward[2], 1, 2)])
    return jnp.concatenate([forward, backward], axis=0).astype(jnp.int32)


def draw_betas(key, part):
    rungs = jnp.arange(R, dtype=jnp.float32)
    jitter = jax.random.uniform(jax.random.fold_in(key, 31), (R,), jnp.float32, -0.3, 0.3)
    levels = (rungs + 0.5 + jitter) / jnp.float32(R)
    values = 0.25 * jnp.exp(levels * jnp.log(jnp.float32(6.0)))
    return values.astype(jnp.float32)


def block_levels(stream_key, dims, split, smallest, top_value):
    gain = 1.0
    for axis_at, parts in split:
        draws = jax.random.uniform(jax.random.fold_in(jax.random.fold_in(stream_key, 6), axis_at), (parts,), jnp.float32, smallest / len(split), top_value / len(split))
        gain = gain * jnp.repeat(jnp.exp(draws), dims[axis_at] // parts).reshape((-1,) + (1,) * (len(dims) - 1 - axis_at))
    return gain


def setup_inputs(seed: int = 0) -> dict:
    seeds = jax.random.split(jax.random.key(seed), 6)
    return {
        "spins": draw_spins(jax.random.fold_in(seeds[5], 71), 0),
        "couplings": draw_couplings(jax.random.fold_in(seeds[5], 71), 0),
        "betas": draw_betas(jax.random.fold_in(seeds[5], 71), 0),
        "metro_uniform": jnp.clip(1.0 * jax.random.uniform(seeds[3], (SWEEPS, R, NX, NY, NZ), jnp.float32) ** block_levels(seeds[3], (SWEEPS, R, NX, NY, NZ), ((2, 32), (3, 8)), -0.2, 0.2), 0.0, 1.0).astype(jnp.bfloat16),
        "swap_uniform": jnp.clip(jax.random.uniform(seeds[4], (R // 2,), jnp.float32, 0.8, 1.0), 0.8, 1.0),
    }


soft_width = 0.1
swap_width = 0.25
swap_gain = 64.0


def neighbour_field(bonds, state):
    field = bonds[0] * jnp.roll(state, -1, 0) + bonds[3] * jnp.roll(state, 1, 0)
    field = field + bonds[1] * jnp.roll(state, -1, 1) + bonds[4] * jnp.roll(state, 1, 1)
    field = field + bonds[2] * jnp.roll(state, -1, 2) + bonds[5] * jnp.roll(state, 1, 2)
    return field


def reference(spins, couplings, betas, metro_uniform, swap_uniform):
    bonds = couplings.astype(jnp.float32)
    shape = (NX, NY, NZ)
    parity = (lax.broadcasted_iota(jnp.int32, shape, 0) + lax.broadcasted_iota(jnp.int32, shape, 1)
              + lax.broadcasted_iota(jnp.int32, shape, 2)) % 2

    def one_replica(index):
        state = spins[index]
        inverse = betas[index].astype(jnp.float32)
        for sweep in range(SWEEPS):
            uniform = metro_uniform[sweep, index].astype(jnp.float32)
            for colour in (0, 1):
                current = state.astype(jnp.float32)
                field = neighbour_field(bonds, current)
                accept = jnp.exp(-inverse * jnp.maximum(2.0 * current * field, 0.0))
                weight = jax.nn.sigmoid((accept - uniform) / soft_width)
                flipped = current * (1.0 - 2.0 * weight)
                state = jnp.where(parity == colour, flipped, current).astype(jnp.bfloat16)
        current = state.astype(jnp.float32)
        bond_sum = bonds[0] * current * jnp.roll(current, -1, 0)
        bond_sum = bond_sum + bonds[1] * current * jnp.roll(current, -1, 1)
        bond_sum = bond_sum + bonds[2] * current * jnp.roll(current, -1, 2)
        energy = -jnp.sum(bond_sum) / jnp.float32(NX * NY * NZ)
        return state, energy

    swept, energies = lax.map(one_replica, jnp.arange(R, dtype=jnp.int32))
    first_e = energies[0::2]
    second_e = energies[1::2]
    delta = swap_gain * (betas[0::2] - betas[1::2]) * (first_e - second_e)
    mix = jax.nn.sigmoid((jnp.minimum(delta, 0.0) - jnp.log(swap_uniform)) / swap_width)
    paired = swept.reshape(R // 2, 2, NX, NY, NZ)

    def one_pair(item):
        pair, weight = item
        upper = pair[0].astype(jnp.float32)
        lower = pair[1].astype(jnp.float32)
        new_upper = (1.0 - weight) * upper + weight * lower
        new_lower = (1.0 - weight) * lower + weight * upper
        return jnp.stack([new_upper, new_lower]).astype(jnp.bfloat16)

    mixed = lax.map(one_pair, (paired, mix))
    return mixed.reshape(R, NX, NY, NZ), energies
```

```python
import functools
import math

import jax
import jax.numpy as jnp
from jax import lax
from jax.experimental import pallas as pl
from jax.experimental.pallas import tpu as pltpu
from jax.sharding import PartitionSpec as P

R = 16
CX, CY, NZ = 4, 64, 256
HALF = NZ // 2
PAD = 8
GROUPS = 2
RG = R // GROUPS
LOG2E = math.log2(math.e)
F32 = jnp.float32
BF16 = jnp.bfloat16
VMEM_LIMIT = 24 * 1024 * 1024

swap_width = 0.25
swap_gain = 64.0

VM = pl.BlockSpec(memory_space=pltpu.VMEM)
SM = pl.BlockSpec(memory_space=pltpu.SMEM)
HB = pl.BlockSpec(memory_space=pl.ANY)


def vm(shape, dtype):
    return pltpu.VMEM(shape, dtype)


def params(limit=VMEM_LIMIT):
    return pltpu.CompilerParams(vmem_limit_bytes=limit)


def cost(ops, moved):
    return pl.CostEstimate(flops=ops, bytes_accessed=moved, transcendentals=0)


def split_matrix():
    row = lax.broadcasted_iota(jnp.int32, (NZ, NZ), 0)
    col = lax.broadcasted_iota(jnp.int32, (NZ, NZ), 1)
    wanted = jnp.where(col < HALF, 2 * col, 2 * (col - HALF) + 1)
    return (row == wanted).astype(F32).astype(BF16)


def join_matrix():
    row = lax.broadcasted_iota(jnp.int32, (NZ, NZ), 0)
    col = lax.broadcasted_iota(jnp.int32, (NZ, NZ), 1)
    wanted = jnp.where(row < HALF, 2 * row, 2 * (row - HALF) + 1)
    return (col == wanted).astype(F32).astype(BF16)


def odd_rows(rows=CY):
    return lax.broadcasted_iota(jnp.int32, (rows, HALF), 0) % 2 == 1


def by_colour(even, odd, x, odd_row):
    if x % 2 == 0:
        return jnp.where(odd_row, odd, even), jnp.where(odd_row, even, odd)
    return jnp.where(odd_row, even, odd), jnp.where(odd_row, odd, even)


def split_spins(spins_ref, *refs):
    a0s, a1s = refs[:GROUPS], refs[GROUPS : 2 * GROUPS]
    sends = refs[2 * GROUPS : 6 * GROUPS]
    buf, sems = refs[6 * GROUPS :]
    copies = []
    for g in range(GROUPS):
        copies.append(
            pltpu.make_async_copy(spins_ref.at[pl.ds(g * RG, RG)], buf.at[pl.ds(g * RG, RG)], sems.at[g])
        )
        copies[-1].start()
    matrix = split_matrix()
    odd_row = odd_rows()
    for g in range(GROUPS):
        copies[g].wait()
        a0, a1 = a0s[g], a1s[g]
        xlo, xhi, ylo, yhi = sends[4 * g : 4 * g + 4]

        @pl.loop(0, RG)
        def _(r):
            cells = buf[g * RG + r].reshape(CX * CY, NZ)
            parts = jnp.dot(cells, matrix, preferred_element_type=F32)
            for x in range(CX):
                rows = parts[x * CY : (x + 1) * CY]
                c0, c1 = by_colour(rows[:, :HALF], rows[:, HALF:], x, odd_row)
                a0[r, x, PAD : PAD + CY, :] = c0
                a1[r, x, PAD : PAD + CY, :] = c1
                ylo[r, x : x + 1, :] = c1[:1]
                yhi[r, x : x + 1, :] = c1[CY - 1 :]
                if x == 0:
                    xlo[r] = c1.astype(BF16)
                if x == CX - 1:
                    xhi[r] = c1.astype(BF16)


def send_shapes():
    return [
        jax.ShapeDtypeStruct((RG, CY, HALF), BF16),
        jax.ShapeDtypeStruct((RG, CY, HALF), BF16),
        jax.ShapeDtypeStruct((RG, CX, HALF), F32),
        jax.ShapeDtypeStruct((RG, CX, HALF), F32),
    ]


def state_shape():
    return vm((RG, CX, CY + 2 * PAD, HALF), F32)


def run_split_spins(spins):
    out = pl.pallas_call(
        split_spins,
        out_shape=[state_shape()] * (2 * GROUPS) + send_shapes() * GROUPS,
        in_specs=[HB],
        out_specs=[VM] * (6 * GROUPS),
        scratch_shapes=[pltpu.VMEM((R, CX, CY, NZ), BF16), pltpu.SemaphoreType.DMA((GROUPS,))],
        compiler_params=params(),
        cost_estimate=cost(10**8, 2 * 2**20),
        name="split_spins",
    )(spins)
    a0 = list(out[:GROUPS])
    a1 = list(out[GROUPS : 2 * GROUPS])
    sends = [list(out[2 * GROUPS + 4 * g : 2 * GROUPS + 4 * g + 4]) for g in range(GROUPS)]
    return a0, a1, sends


def split_draws(sweep, with_bonds, *refs):
    refs = list(refs)
    bonds_ref = refs.pop(0) if with_bonds else None
    uniform_ref = refs.pop(0)
    u0s, u1s = refs[:GROUPS], refs[GROUPS : 2 * GROUPS]
    del refs[: 2 * GROUPS]
    outs = [refs.pop(0), refs.pop(0)] if with_bonds else None
    bond_buf = refs.pop(0) if with_bonds else None
    buf, sems = refs
    copies = []
    if with_bonds:
        bond_copy = pltpu.make_async_copy(bonds_ref, bond_buf, sems.at[GROUPS])
        bond_copy.start()
    for g in range(GROUPS):
        copies.append(
            pltpu.make_async_copy(uniform_ref.at[sweep, pl.ds(g * RG, RG)], buf.at[pl.ds(g * RG, RG)], sems.at[g])
        )
        copies[-1].start()
    matrix = split_matrix()
    odd_row = odd_rows()
    if with_bonds:
        bond_copy.wait()
        for x in range(CX):
            halves = []
            for k in range(6):
                cells = bond_buf[k, x].astype(F32).astype(BF16)
                parts = jnp.dot(cells, matrix, preferred_element_type=F32)
                halves.append((parts[:, :HALF], parts[:, HALF:]))
            for place, k in enumerate((0, 3, 1, 4)):
                c0, c1 = by_colour(*halves[k], x, odd_row)
                outs[0][place, x] = c0
                outs[1][place, x] = c1
            for place, (k, m) in enumerate(((2, 5), (5, 2))):
                c0, c1 = by_colour(halves[k][0], halves[m][1], x, odd_row)
                outs[0][4 + place, x] = c0
                outs[1][4 + place, x] = c1
    for g in range(GROUPS):
        copies[g].wait()
        u0, u1 = u0s[g], u1s[g]

        @pl.loop(0, RG)
        def _(r):
            cells = buf[g * RG + r].reshape(CX * CY, NZ)
            parts = jnp.dot(cells, matrix, preferred_element_type=F32) * 5.0
            for x in range(CX):
                rows = parts[x * CY : (x + 1) * CY]
                c0, c1 = by_colour(rows[:, :HALF], rows[:, HALF:], x, odd_row)
                u0[r, x] = c0
                u1[r, x] = c1


def run_split_draws(sweep, couplings, uniform):
    with_bonds = couplings is not None
    bond_out = [vm((6, CX, CY, HALF), F32)] * 2 if with_bonds else []
    bond_scratch = [pltpu.VMEM((6, CX, CY, NZ), jnp.int32)] if with_bonds else []
    out = pl.pallas_call(
        functools.partial(split_draws, sweep, with_bonds),
        out_shape=[vm((RG, CX, CY, HALF), F32)] * (2 * GROUPS) + bond_out,
        in_specs=[HB] * (2 if with_bonds else 1),
        out_specs=[VM] * (2 * GROUPS + len(bond_out)),
        scratch_shapes=bond_scratch
        + [pltpu.VMEM((R, CX, CY, NZ), BF16), pltpu.SemaphoreType.DMA((GROUPS + 1,))],
        compiler_params=params(),
        cost_estimate=cost(10**8, 2 * 2**20),
        name=f"split_draws_{sweep}",
    )(*([couplings] if with_bonds else []), uniform)
    return list(out[:GROUPS]), list(out[GROUPS : 2 * GROUPS]), list(out[2 * GROUPS :])


def half_sweep(colour, last, scale_ref, own_in, other_in, u_ref, bonds_ref, xlo_ref, xhi_ref, ylo_ref, yhi_ref, *outs):
    own, other = outs[:2]
    if last:
        energy = outs[2]
    else:
        sxlo, sxhi, sylo, syhi = outs[2:]

    @pl.loop(0, RG)
    def _(r):
        for x in range(CX):
            other[r, x, PAD - 1 : PAD, :] = ylo_ref[r, x : x + 1, :]
            other[r, x, PAD + CY : PAD + CY + 1, :] = yhi_ref[r, x : x + 1, :]

    tile = 16
    odd_row = odd_rows(tile)

    @pl.loop(0, RG // 2)
    def _(pair):
        sums = [jnp.zeros((tile, HALF), F32) for _ in range(2)]
        for x in range(CX):
            for y in range(0, CY, tile):
                bonds = [bonds_ref[k, x, y : y + tile, :] for k in range(6)]
                for i in range(2):
                    r = pair * 2 + i

                    def near(dx, dy):
                        at = x + dx
                        if at < 0:
                            return xlo_ref[r, y : y + tile, :].astype(F32)
                        if at >= CX:
                            return xhi_ref[r, y : y + tile, :].astype(F32)
                        return other[r, at, PAD + y + dy : PAD + y + dy + tile, :]

                    same = near(0, 0)
                    below, above = pltpu.roll(same, 1, 1), pltpu.roll(same, HALF - 1, 1)
                    if (colour + x) % 2 == 0:
                        beside = jnp.where(odd_row, above, below)
                    else:
                        beside = jnp.where(odd_row, below, above)
                    field = bonds[0] * near(1, 0) + bonds[1] * near(-1, 0)
                    field = field + (bonds[2] * near(0, 1) + bonds[3] * near(0, -1))
                    field = field + (bonds[4] * same + bonds[5] * beside)
                    spin = own[r, x, PAD + y : PAD + y + tile, :]
                    accept = jnp.exp2(jnp.minimum(spin * field * scale_ref[r], 0.0))
                    new = (spin * jnp.tanh(u_ref[r, x, y : y + tile, :] - 5.0 * accept)).astype(BF16)
                    wide = new.astype(F32)
                    own[r, x, PAD + y : PAD + y + tile, :] = wide
                    if last:
                        sums[i] = sums[i] + wide * field
                    else:
                        if x == 0:
                            sxlo[r, y : y + tile, :] = new
                        if x == CX - 1:
                            sxhi[r, y : y + tile, :] = new
                        if y == 0:
                            sylo[r, x : x + 1, :] = wide[:1]
                        if y == CY - tile:
                            syhi[r, x : x + 1, :] = wide[tile - 1 :]
        if last:
            for i in range(2):
                energy[pair * 2 + i] = sums[i][:8] + sums[i][8:]


def run_half_sweep(colour, last, scale, own, other, u, bonds, halos, name):
    extra = [jax.ShapeDtypeStruct((RG, 8, HALF), F32)] if last else send_shapes()
    out = pl.pallas_call(
        functools.partial(half_sweep, colour, last),
        out_shape=[state_shape()] * 2 + extra,
        in_specs=[SM] + [VM] * 8,
        out_specs=[VM] * (2 + len(extra)),
        input_output_aliases={1: 0, 2: 1},
        compiler_params=params(),
        cost_estimate=cost(10**8, 2 * 2**20),
        name=name,
    )(scale, own, other, u, bonds, *halos)
    return out[0], out[1], list(out[2:])


def mix_and_join(mix_ref, *refs):
    a0s, a1s = refs[:GROUPS], refs[GROUPS : 2 * GROUPS]
    out_ref, buf, sems = refs[2 * GROUPS :]
    matrix = join_matrix()
    odd_row = odd_rows()
    copies = []
    for g in range(GROUPS):

        @pl.loop(0, RG // 2)
        def _(pair):
            weight = mix_ref[g * (RG // 2) + pair]
            keep = 1.0 - weight
            r = pair * 2
            for x in range(CX):
                new = [[], []]
                for state in (a0s[g], a1s[g]):
                    upper = state[r, x, PAD : PAD + CY, :]
                    lower = state[r + 1, x, PAD : PAD + CY, :]
                    new[0].append(keep * upper + weight * lower)
                    new[1].append(keep * lower + weight * upper)
                for i in range(2):
                    even, odd = by_colour(*new[i], x, odd_row)
                    cells = jnp.concatenate([even.astype(BF16), odd.astype(BF16)], axis=1)
                    buf[g * RG + r + i, x] = jnp.dot(cells, matrix, preferred_element_type=F32).astype(BF16)

        copies.append(
            pltpu.make_async_copy(buf.at[pl.ds(g * RG, RG)], out_ref.at[pl.ds(g * RG, RG)], sems.at[g])
        )
        copies[-1].start()
    for copy in copies:
        copy.wait()


def run_mix_and_join(mix, a0, a1):
    return pl.pallas_call(
        mix_and_join,
        out_shape=jax.ShapeDtypeStruct((R, CX, CY, NZ), BF16),
        in_specs=[SM] + [VM] * (2 * GROUPS),
        out_specs=HB,
        scratch_shapes=[pltpu.VMEM((R, CX, CY, NZ), BF16), pltpu.SemaphoreType.DMA((GROUPS,))],
        compiler_params=params(),
        cost_estimate=cost(10**8, 2 * 2**20),
        name="mix_and_join",
    )(mix, *a0, *a1)


def shift(x, axis, by):
    count = lax.axis_size(axis)
    return lax.ppermute(x, axis, [(i, (i + by) % count) for i in range(count)])


def exchange(sends):
    xlo, xhi, ylo, yhi = sends
    return [shift(xhi, "gx", 1), shift(xlo, "gx", -1), shift(yhi, "gy", 1), shift(ylo, "gy", -1)]


def body(spins, couplings, betas, metro_uniform, swap_uniform):
    a0, a1, sends = run_split_spins(spins)
    halos = [exchange(s) for s in sends]
    u, bonds = {}, None
    u[0, 0], u[0, 1], bonds = run_split_draws(0, couplings, metro_uniform)
    u[1, 0], u[1, 1], _ = run_split_draws(1, None, metro_uniform)
    scale = (-2.0 * LOG2E) * betas
    states = [a0, a1]
    sums = [None] * GROUPS
    for sweep in range(2):
        for colour in (0, 1):
            last = sweep == 1 and colour == 1
            for g in range(GROUPS):
                own, other, rest = run_half_sweep(
                    colour,
                    last,
                    scale[g * RG : (g + 1) * RG],
                    states[colour][g],
                    states[1 - colour][g],
                    u[sweep, colour][g],
                    bonds[colour],
                    halos[g],
                    f"half_sweep_{sweep}{colour}{g}",
                )
                states[colour][g], states[1 - colour][g] = own, other
                if last:
                    sums[g] = rest[0]
                else:
                    halos[g] = exchange(rest)
    partial_sum = jnp.sum(jnp.concatenate(sums, axis=0), axis=(1, 2))
    both = ("gx", "gy")
    count = lax.axis_size(both)
    copies = jnp.broadcast_to(partial_sum[None], (count, R))
    total = jnp.sum(lax.all_to_all(copies, both, 0, 0), axis=0)
    cell_count = CX * CY * NZ * count
    energies = -total / jnp.float32(cell_count)
    delta = swap_gain * (betas[0::2] - betas[1::2]) * (energies[0::2] - energies[1::2])
    mix = jax.nn.sigmoid((jnp.minimum(delta, 0.0) - jnp.log(swap_uniform)) / swap_width)
    return run_mix_and_join(mix, *states), energies


def solution(mesh):
    return jax.shard_map(
        body,
        mesh=mesh,
        in_specs=(
            P(None, "gx", "gy", None),
            P(None, "gx", "gy", None),
            P(),
            P(None, None, "gx", "gy", None),
            P(),
        ),
        out_specs=(P(None, "gx", "gy", None), P()),
        check_vma=False,
    )
```

```python
import functools
import math

import jax
import jax.numpy as jnp
from jax import lax
from jax.experimental import pallas as pl
from jax.experimental.pallas import tpu as pltpu
from jax.sharding import PartitionSpec as P

R = 16
CX, CY, NZ = 4, 64, 256
HALF = NZ // 2
PAD = 8
UNROLL = 4
OUTER, INNER = (0, CX - 1), (1, 2)
LOG2E = math.log2(math.e)
F32 = jnp.float32
BF16 = jnp.bfloat16
MIB = 1024 * 1024

swap_width = 0.25
swap_gain = 64.0

VM = pl.BlockSpec(memory_space=pltpu.VMEM)
SM = pl.BlockSpec(memory_space=pltpu.SMEM)
HB = pl.BlockSpec(memory_space=pltpu.HBM)


def in_hbm(x):
    return pltpu.with_memory_space_constraint(x, pltpu.HBM)


def split_matrix():
    row = lax.broadcasted_iota(jnp.int32, (NZ, NZ), 0)
    col = lax.broadcasted_iota(jnp.int32, (NZ, NZ), 1)
    wanted = jnp.where(col < HALF, 2 * col, 2 * (col - HALF) + 1)
    return (row == wanted).astype(F32).astype(BF16)


def join_matrix():
    row = lax.broadcasted_iota(jnp.int32, (NZ, NZ), 0)
    col = lax.broadcasted_iota(jnp.int32, (NZ, NZ), 1)
    wanted = jnp.where(row < HALF, 2 * row, 2 * (row - HALF) + 1)
    return (col == wanted).astype(F32).astype(BF16)


def odd_rows(rows=CY):
    return lax.broadcasted_iota(jnp.int32, (rows, HALF), 0) % 2 == 1


def by_colour(even, odd, x, odd_row):
    if x % 2 == 0:
        return jnp.where(odd_row, odd, even), jnp.where(odd_row, even, odd)
    return jnp.where(odd_row, even, odd), jnp.where(odd_row, odd, even)


def send_layers(side_ref, own, xeven, xodd):
    layer = (CX - 1) * (1 - side_ref[0])

    for r in range(R):
        xeven[r] = own[r, layer, PAD : PAD + CY, :].astype(BF16)
        xodd[r] = own[r, CX - 1 - layer, PAD : PAD + CY, :].astype(BF16)


def send_rows(side_ref, own, yeven, yodd):
    lower = side_ref[1] == 0
    for r in range(R):
        for x in range(CX):
            first = own[r, x, PAD : PAD + 1, :]
            final = own[r, x, PAD + CY - 1 : PAD + CY, :]
            yeven[r, x : x + 1, :] = jnp.where(lower, final, first)
            yodd[r, x : x + 1, :] = jnp.where(lower, first, final)


STATE = pltpu.VMEM((R, CX, CY + 2 * PAD, HALF), F32)
DRAWS = pltpu.VMEM((R, CX, CY, HALF), F32)
BONDS = pltpu.VMEM((6, CX, CY, HALF), F32)
LAYER = jax.ShapeDtypeStruct((R, CY, HALF), BF16)
ROWS = jax.ShapeDtypeStruct((R, CX, HALF), F32)


def call(kernel, name, outs, in_specs, out_specs, scratch=(), aliases={}, limit=8, flops=10**7):
    return pl.pallas_call(
        kernel,
        out_shape=outs,
        in_specs=in_specs,
        out_specs=out_specs,
        scratch_shapes=list(scratch),
        input_output_aliases=aliases,
        compiler_params=pltpu.CompilerParams(vmem_limit_bytes=limit * MIB),
        cost_estimate=pl.CostEstimate(flops=flops, bytes_accessed=2 * MIB, transcendentals=0),
        name=name,
    )


def split_outer(side_ref, spins_ref, a0, a1, xeven, xodd, yeven, yodd, layers, edge_rows, split_rows, sems):
    copies = []
    for i, x in enumerate(OUTER):
        copies.append(pltpu.make_async_copy(spins_ref.at[:, x], layers.at[i], sems.at[i]))
    for i, y in enumerate((0, CY - 8)):
        copies.append(
            pltpu.make_async_copy(
                spins_ref.at[:, pl.ds(1, 2), pl.ds(y, 8)], edge_rows.at[i], sems.at[2 + i]
            )
        )
    for copy in copies:
        copy.start()
    matrix = split_matrix()
    odd_row = odd_rows()
    for i, x in enumerate(OUTER):
        copies[i].wait()

        cells = layers[i].reshape(R * CY, NZ)
        parts = jnp.dot(cells, matrix, preferred_element_type=F32)
        for r in range(R):
            rows = parts[r * CY : (r + 1) * CY]
            c0, c1 = by_colour(rows[:, :HALF], rows[:, HALF:], x, odd_row)
            a0[r, x, PAD : PAD + CY, :] = c0
            a1[r, x, PAD : PAD + CY, :] = c1

    for i in range(2):
        copies[2 + i].wait()
        cells = edge_rows[i].reshape(R * 2 * 8, NZ)
        split_rows[i] = jnp.dot(cells, matrix, preferred_element_type=F32).reshape(R, 2, 8, NZ)
    send_layers(side_ref, a1, xeven, xodd)
    lower = side_ref[1] == 0
    for r in range(R):
        for x in range(CX):
            if x in OUTER:
                first = a1[r, x, PAD : PAD + 1, :]
                final = a1[r, x, PAD + CY - 1 : PAD + CY, :]
            else:
                at = 0 if x % 2 == 1 else HALF
                first = split_rows[0, r, x - 1, 0:1, at : at + HALF]
                at = HALF - at
                final = split_rows[1, r, x - 1, 7:8, at : at + HALF]
            yeven[r, x : x + 1, :] = jnp.where(lower, final, first)
            yodd[r, x : x + 1, :] = jnp.where(lower, first, final)


def run_split_outer(side, spins):
    return call(
        split_outer,
        "split_outer",
        [STATE] * 2 + [LAYER] * 2 + [ROWS] * 2,
        [SM, HB],
        [VM] * 6,
        [
            pltpu.VMEM((2, R, CY, NZ), BF16),
            pltpu.VMEM((2, R, 2, 8, NZ), BF16),
            pltpu.VMEM((2, R, 2, 8, NZ), F32),
            pltpu.SemaphoreType.DMA((4,)),
        ],
    )(side, in_hbm(spins))


def split_field(buf, u0, u1, matrix, odd_row):
    @pl.loop(0, R, step=4)
    def _(first):
        cells = buf[pl.ds(first, 4)].reshape(4 * CX * CY, NZ)
        parts = jnp.dot(cells, matrix, preferred_element_type=F32) * 5.0
        for k in range(4 * CX):
            rows = parts[k * CY : (k + 1) * CY]
            r, x = first + k // CX, k % CX
            c0, c1 = by_colour(rows[:, :HALF], rows[:, HALF:], x, odd_row)
            u0[r, x] = c0
            u1[r, x] = c1


def split_inner(
    spins_ref, couplings_ref, uniform_ref, a0_in, a1_in, a0, a1, u0, u1, bonds0, bonds1, layers, bond_buf, buf, sems
):
    copies = [
        pltpu.make_async_copy(spins_ref.at[:, pl.ds(1, 2)], layers, sems.at[0]),
        pltpu.make_async_copy(couplings_ref, bond_buf, sems.at[1]),
        pltpu.make_async_copy(uniform_ref.at[0], buf, sems.at[2]),
    ]
    for copy in copies:
        copy.start()
    matrix = split_matrix()
    odd_row = odd_rows()
    copies[0].wait()

    @pl.loop(0, R, step=8)
    def _(first):
        cells = layers[pl.ds(first, 8)].reshape(16 * CY, NZ)
        parts = jnp.dot(cells, matrix, preferred_element_type=F32)
        for k in range(16):
            rows = parts[k * CY : (k + 1) * CY]
            x = 1 + k % 2
            c0, c1 = by_colour(rows[:, :HALF], rows[:, HALF:], x, odd_row)
            a0[first + k // 2, x, PAD : PAD + CY, :] = c0
            a1[first + k // 2, x, PAD : PAD + CY, :] = c1

    copies[1].wait()
    for x in range(CX):
        halves = []
        for k in range(6):
            cells = bond_buf[k, x].astype(F32).astype(BF16)
            parts = jnp.dot(cells, matrix, preferred_element_type=F32)
            halves.append((parts[:, :HALF], parts[:, HALF:]))
        for place, k in enumerate((0, 3, 1, 4)):
            bonds0[place, x], bonds1[place, x] = by_colour(*halves[k], x, odd_row)
        for place, (k, m) in enumerate(((2, 5), (5, 2))):
            bonds0[4 + place, x], bonds1[4 + place, x] = by_colour(halves[k][0], halves[m][1], x, odd_row)
    copies[2].wait()
    split_field(buf, u0, u1, matrix, odd_row)


def run_split_inner(spins, couplings, uniform, a0, a1):
    return call(
        split_inner,
        "split_inner",
        [STATE] * 2 + [DRAWS] * 2 + [BONDS] * 2,
        [HB] * 3 + [VM] * 2,
        [VM] * 6,
        [
            pltpu.VMEM((R, 2, CY, NZ), BF16),
            pltpu.VMEM((6, CX, CY, NZ), jnp.int32),
            pltpu.VMEM((R, CX, CY, NZ), BF16),
            pltpu.SemaphoreType.DMA((3,)),
        ],
        {3: 0, 4: 1},
    )(in_hbm(spins), in_hbm(couplings), in_hbm(uniform), a0, a1)


def split_draws(uniform_ref, u0, u1, buf, sem):
    copy = pltpu.make_async_copy(uniform_ref.at[1], buf, sem)
    copy.start()
    matrix = split_matrix()
    odd_row = odd_rows()
    copy.wait()
    split_field(buf, u0, u1, matrix, odd_row)


def run_split_draws(uniform):
    return call(
        split_draws,
        "split_draws",
        [DRAWS] * 2,
        [HB],
        [VM] * 2,
        [pltpu.VMEM((R, CX, CY, NZ), BF16), pltpu.SemaphoreType.DMA],
    )(in_hbm(uniform))


def put_rows(side_ref, other, yeven, yodd):
    lower = side_ref[1] == 0
    for r in range(R):
        for x in range(CX):
            even, odd = yeven[r, x : x + 1, :], yodd[r, x : x + 1, :]
            other[r, x, PAD - 1 : PAD, :] = jnp.where(lower, odd, even)
            other[r, x, PAD + CY : PAD + CY + 1, :] = jnp.where(lower, even, odd)


def put_layers(side_ref, beyond, xeven, xodd):
    upper = side_ref[0]
    for r in range(R):
        beyond[1 - upper, r] = xeven[r].astype(F32)
        beyond[upper, r] = xodd[r].astype(F32)


def update(colour, layers, betas_ref, own, other, u_ref, bonds_ref, beyond, energy):
    tile = 16
    odd_row = odd_rows(tile)

    @pl.loop(0, R, step=UNROLL)
    def _(first):
        sums = [jnp.zeros((tile, HALF), F32) for _ in range(UNROLL)]
        scales = [betas_ref[first + i] * (-2.0 * LOG2E) for i in range(UNROLL)]
        for x in layers:
            for y in range(0, CY, tile):
                bonds = [bonds_ref[k, x, y : y + tile, :] for k in range(6)]
                for i in range(UNROLL):
                    r = first + i

                    def near(dx, dy):
                        at = x + dx
                        if at < 0:
                            return beyond[0, r, y : y + tile, :]
                        if at >= CX:
                            return beyond[1, r, y : y + tile, :]
                        return other[r, at, PAD + y + dy : PAD + y + dy + tile, :]

                    same = near(0, 0)
                    below, above = pltpu.roll(same, 1, 1), pltpu.roll(same, HALF - 1, 1)
                    if (colour + x) % 2 == 0:
                        beside = jnp.where(odd_row, above, below)
                    else:
                        beside = jnp.where(odd_row, below, above)
                    field = bonds[0] * near(1, 0) + bonds[1] * near(-1, 0)
                    field = field + (bonds[2] * near(0, 1) + bonds[3] * near(0, -1))
                    field = field + (bonds[4] * same + bonds[5] * beside)
                    spin = own[r, x, PAD + y : PAD + y + tile, :]
                    accept = jnp.exp2(jnp.minimum(spin * field * scales[i], 0.0))
                    new = spin * jnp.tanh(u_ref[r, x, y : y + tile, :] - 5.0 * accept)
                    wide = new.astype(BF16).astype(F32)
                    own[r, x, PAD + y : PAD + y + tile, :] = wide
                    if energy is not None:
                        sums[i] = sums[i] + wide * field
        if energy is not None:
            for i in range(UNROLL):
                energy[first + i] = sums[i][:8] + sums[i][8:]


def sweep_outer(colour, side_ref, betas_ref, own_in, other_in, u, bonds, xe, xo, ye, yo, own, other, sxe, sxo, beyond):
    put_layers(side_ref, beyond, xe, xo)
    put_rows(side_ref, other, ye, yo)
    update(colour, OUTER, betas_ref, own, other, u, bonds, beyond, None)
    send_layers(side_ref, own, sxe, sxo)


def sweep_inner(colour, side_ref, betas_ref, own_in, other_in, u, bonds, own, other, sye, syo):
    update(colour, INNER, betas_ref, own, other, u, bonds, None, None)
    send_rows(side_ref, own, sye, syo)


BEYOND = pltpu.VMEM((2, R, CY, HALF), F32)
ENERGY = jax.ShapeDtypeStruct((R, 8, HALF), F32)


def final_inner(side_ref, betas_ref, own_in, other_in, u, bonds, ye, yo, own, other, energy):
    put_rows(side_ref, other, ye, yo)
    update(1, INNER, betas_ref, own, other, u, bonds, None, energy)


def final_outer(side_ref, betas_ref, own_in, other_in, u, bonds, xe, xo, inner_energy, own, other, sums_ref, beyond, energy):
    put_layers(side_ref, beyond, xe, xo)
    update(1, OUTER, betas_ref, own, other, u, bonds, beyond, energy)
    lines = jnp.sum(energy[...] + inner_energy[...], axis=1)
    totals = jnp.sum(lines, axis=1, keepdims=True)
    diagonal = lax.broadcasted_iota(jnp.int32, (R, R), 0) == lax.broadcasted_iota(jnp.int32, (R, R), 1)
    row = jnp.sum(jnp.where(diagonal, totals, 0.0), axis=0, keepdims=True)
    sums_ref[...] = jnp.broadcast_to(row[None], sums_ref.shape)


def run_sweep_outer(colour, name, side, betas, own, other, u, bonds, xs, ys):
    return call(
        functools.partial(sweep_outer, colour),
        name,
        [STATE] * 2 + [LAYER] * 2,
        [SM, SM] + [VM] * 8,
        [VM] * 4,
        [BEYOND],
        {2: 0, 3: 1},
    )(side, betas, own, other, u, bonds, *xs, *ys)


def run_sweep_inner(colour, name, side, betas, own, other, u, bonds):
    return call(
        functools.partial(sweep_inner, colour),
        name,
        [STATE] * 2 + [ROWS] * 2,
        [SM, SM] + [VM] * 4,
        [VM] * 4,
        (),
        {2: 0, 3: 1},
    )(side, betas, own, other, u, bonds)


def run_final_inner(side, betas, own, other, u, bonds, ys):
    return call(
        final_inner,
        "final_inner",
        [STATE] * 2 + [ENERGY],
        [SM, SM] + [VM] * 6,
        [VM] * 3,
        (),
        {2: 0, 3: 1},
    )(side, betas, own, other, u, bonds, *ys)


def run_final_outer(count, side, betas, own, other, u, bonds, xs, energy):
    return call(
        final_outer,
        "final_outer",
        [STATE] * 2 + [pltpu.VMEM((count, 1, R), F32)],
        [SM, SM] + [VM] * 7,
        [VM] * 3,
        [BEYOND, pltpu.VMEM((R, 8, HALF), F32)],
        {2: 0, 3: 1},
    )(side, betas, own, other, u, bonds, *xs, energy)


def mix_and_join(cell_count, betas_ref, swap_ref, sums_ref, a0, a1, out_ref, energies_ref, weights, buf, sems):
    total = jnp.sum(sums_ref[:, 0, :], axis=0, keepdims=True)
    energies = -total / cell_count
    energies_ref[...] = energies
    place = lax.broadcasted_iota(jnp.int32, (1, R), 1)
    betas = jnp.zeros((1, R), F32)
    draws = jnp.ones((1, R), F32)
    for r in range(R):
        betas = jnp.where(place == r, betas_ref[r], betas)
    for k in range(R // 2):
        draws = jnp.where(place == 2 * k, swap_ref[k], draws)
    beta_step = betas[:, : R - 1] - betas[:, 1:]
    energy_step = energies[:, : R - 1] - energies[:, 1:]
    delta = swap_gain * beta_step * energy_step
    mix = jax.nn.sigmoid((jnp.minimum(delta, 0.0) - jnp.log(draws[:, : R - 1])) / swap_width)
    for k in range(R // 2):
        weights[k : k + 1, :] = jnp.broadcast_to(mix[:, 2 * k : 2 * k + 1], (1, HALF))
    matrix = join_matrix()
    odd_row = odd_rows()

    def out_copy(pair):
        at = pl.ds(pair * 2, 2)
        return pltpu.make_async_copy(buf.at[at], out_ref.at[at], sems.at[pair])

    @pl.loop(0, R // 2)
    def _(pair):
        weight = jnp.broadcast_to(weights[pl.ds(pair, 1), :], (CY, HALF))
        r = pair * 2
        cells = [[], []]
        for x in range(CX):
            new = [[], []]
            for state in (a0, a1):
                upper = state[r, x, PAD : PAD + CY, :]
                lower = state[r + 1, x, PAD : PAD + CY, :]
                moved = weight * (lower - upper)
                new[0].append(upper + moved)
                new[1].append(lower - moved)
            for i in range(2):
                even, odd = by_colour(*new[i], x, odd_row)
                cells[i].append(jnp.concatenate([even.astype(BF16), odd.astype(BF16)], axis=1))
        for i in range(2):
            joined = jnp.dot(jnp.concatenate(cells[i], axis=0), matrix, preferred_element_type=F32)
            buf[r + i] = joined.astype(BF16).reshape(CX, CY, NZ)
        out_copy(pair).start()

    @pl.loop(0, R // 2)
    def _(pair):
        out_copy(pair).wait()


def run_mix_and_join(cell_count, betas, swap, sums, a0, a1):
    return call(
        functools.partial(mix_and_join, cell_count),
        "mix_and_join",
        [jax.ShapeDtypeStruct((R, CX, CY, NZ), BF16), jax.ShapeDtypeStruct((1, R), F32)],
        [SM] * 2 + [VM] * 3,
        [HB, VM],
        [
            pltpu.VMEM((R // 2, HALF), F32),
            pltpu.VMEM((R, CX, CY, NZ), BF16),
            pltpu.SemaphoreType.DMA((R // 2,)),
        ],
    )(betas, swap, sums, a0, a1)


def swap_pairs(x, axis, odd):
    count = lax.axis_size(axis)
    return lax.ppermute(x, axis, [(i, (((i + odd) ^ 1) - odd) % count) for i in range(count)])


def exchange(axis, even, odd):
    return [swap_pairs(even, axis, 0), swap_pairs(odd, axis, 1)]


def body(spins, couplings, betas, metro_uniform, swap_uniform):
    side = jnp.stack([lax.axis_index("gx") % 2, lax.axis_index("gy") % 2]).astype(jnp.int32)
    a0, a1, xe, xo, ye, yo = run_split_outer(side, spins)
    xs, ys = exchange("gx", xe, xo), exchange("gy", ye, yo)
    a0, a1, u00, u01, bonds0, bonds1 = run_split_inner(spins, couplings, metro_uniform, a0, a1)
    u10, u11 = run_split_draws(metro_uniform)
    states = [a0, a1]
    for step, (u, bonds) in enumerate(((u00, bonds0), (u01, bonds1), (u10, bonds0))):
        colour = step % 2
        own, other = states[colour], states[1 - colour]
        own, other, xe, xo = run_sweep_outer(colour, f"sweep_outer_{step}", side, betas, own, other, u, bonds, xs, ys)
        xs = exchange("gx", xe, xo)
        own, other, ye, yo = run_sweep_inner(colour, f"sweep_inner_{step}", side, betas, own, other, u, bonds)
        ys = exchange("gy", ye, yo)
        states[colour], states[1 - colour] = own, other
    both = ("gx", "gy")
    count = lax.axis_size(both)
    a0, a1 = states
    a1, a0, energy = run_final_inner(side, betas, a1, a0, u11, bonds1, ys)
    a1, a0, sums = run_final_outer(count, side, betas, a1, a0, u11, bonds1, xs, energy)
    sums = lax.all_to_all(sums, both, 0, 0, tiled=True)
    cell_count = float(CX * CY * NZ * count)
    out, energies = run_mix_and_join(
        cell_count, betas, swap_uniform, sums, a0, a1
    )
    return out, energies[0]


def solution(mesh):
    return jax.shard_map(
        body,
        mesh=mesh,
        in_specs=(
            P(None, "gx", "gy", None),
            P(None, "gx", "gy", None),
            P(),
            P(None, None, "gx", "gy", None),
            P(),
        ),
        out_specs=(P(None, "gx", "gy", None), P()),
        check_vma=False,
    )
```

```python
import functools
import math

import jax
import jax.numpy as jnp
from jax import lax
from jax.experimental import pallas as pl
from jax.experimental.pallas import tpu as pltpu
from jax.sharding import PartitionSpec as P


R = 16
CX, CY, NZ = 4, 64, 256
HALF = NZ // 2
PAD = 8
UNROLL = 4
PAIRS = 2
FIRST, LAST, OUTER, INNER = (0,), (CX - 1,), (0, CX - 1), (1, 2)
FLIP, UPPER, BETAS, DRAWN, TABLE_ROWS = R, R + 1, R + 2, R + 3, R + 8
LOG2E = math.log2(math.e)
F32 = jnp.float32
BF16 = jnp.bfloat16
MIB = 1024 * 1024

swap_width = 0.25
swap_gain = 64.0

VM = pl.BlockSpec(memory_space=pltpu.VMEM)
SM = pl.BlockSpec(memory_space=pltpu.SMEM)
HB = pl.BlockSpec(memory_space=pltpu.HBM)


def in_hbm(x):
    return pltpu.with_memory_space_constraint(x, pltpu.HBM)


def split_matrix():
    row = lax.broadcasted_iota(jnp.int32, (NZ, NZ), 0)
    col = lax.broadcasted_iota(jnp.int32, (NZ, NZ), 1)
    wanted = jnp.where(col < HALF, 2 * col, 2 * (col - HALF) + 1)
    return (row == wanted).astype(F32).astype(BF16)


def join_matrix():
    row = lax.broadcasted_iota(jnp.int32, (NZ, NZ), 0)
    col = lax.broadcasted_iota(jnp.int32, (NZ, NZ), 1)
    wanted = jnp.where(row < HALF, 2 * row, 2 * (row - HALF) + 1)
    return (col == wanted).astype(F32).astype(BF16)


def device_side():
    return lax.axis_index("gx") % 2, lax.axis_index("gy") % 2


def fill_table(side, betas_ref, swap_ref, table):
    place = lax.broadcasted_iota(jnp.int32, (1, HALF), 1)
    betas = jnp.zeros((1, HALF), F32)
    drawn = jnp.ones((1, HALF), F32)
    for r in range(R):
        table[r : r + 1, :] = jnp.full((1, HALF), betas_ref[r] * (-2.0 * LOG2E), F32)
        betas = jnp.where(place == r, betas_ref[r], betas)
    for k in range(R // 2):
        drawn = jnp.where(place == 2 * k, swap_ref[k], drawn)
    for i in range(2):
        table[R + i : R + i + 1, :] = jnp.full((1, HALF), side[i], jnp.int32).astype(F32)
    table[BETAS : BETAS + 1, :] = betas
    table[DRAWN : DRAWN + 1, :] = drawn


def odd_rows_of(table, rows):
    place = lax.broadcasted_iota(jnp.int32, (rows, HALF), 0) % 2
    return place.astype(F32) != jnp.broadcast_to(table[FLIP : FLIP + 1, :], (rows, HALF))


def odd_rows(side, rows=CY):
    return (lax.broadcasted_iota(jnp.int32, (rows, HALF), 0) + side[0]) % 2 == 1


def layer_at(side, x):
    return jnp.where(side[0] == 0, x, CX - 1 - x)


def by_colour(even, odd, x, odd_row):
    if x % 2 == 0:
        return jnp.where(odd_row, odd, even), jnp.where(odd_row, even, odd)
    return jnp.where(odd_row, even, odd), jnp.where(odd_row, odd, even)


def send_rows(table, own, yeven, yodd):
    lower = table[UPPER : UPPER + 1, :] == 0.0
    for r in range(R):
        for x in range(CX):
            first = own[r, x, PAD : PAD + 1, :]
            final = own[r, x, PAD + CY - 1 : PAD + CY, :]
            yeven[r, x : x + 1, :] = jnp.where(lower, final, first)
            yodd[r, x : x + 1, :] = jnp.where(lower, first, final)


STATE = pltpu.VMEM((R, CX, CY + 2 * PAD, HALF), F32)
DRAWS = pltpu.VMEM((R, CX, CY, HALF), F32)
BONDS = pltpu.VMEM((6, CX, CY, HALF), F32)
LAYER = jax.ShapeDtypeStruct((R, CY, HALF), BF16)
ROWS = jax.ShapeDtypeStruct((R, CX, HALF), F32)
TABLE = jax.ShapeDtypeStruct((TABLE_ROWS, HALF), F32)


def call(kernel, outs, in_specs, out_specs, scratch=(), aliases={}, limit=8, flops=10**7):
    return pl.pallas_call(
        kernel,
        out_shape=outs,
        in_specs=in_specs,
        out_specs=out_specs,
        scratch_shapes=list(scratch),
        input_output_aliases=aliases,
        compiler_params=pltpu.CompilerParams(vmem_limit_bytes=limit * MIB),
        cost_estimate=pl.CostEstimate(flops=flops, bytes_accessed=2 * MIB, transcendentals=0),
    )


def split_outer(spins_ref, a0, a1, xeven, xodd, yeven, yodd, layers, edge_rows, split_rows, sems):
    side = device_side()
    copies = []
    for i, x in enumerate(OUTER):
        copies.append(pltpu.make_async_copy(spins_ref.at[:, layer_at(side, x)], layers.at[i], sems.at[i]))
    for i, y in enumerate((0, CY - 8)):
        copies.append(
            pltpu.make_async_copy(
                spins_ref.at[:, pl.ds(1, 2), pl.ds(y, 8)], edge_rows.at[i], sems.at[2 + i]
            )
        )
    for copy in copies:
        copy.start()
    matrix = split_matrix()
    odd_row = odd_rows(side)
    for i, x in enumerate(OUTER):
        copies[i].wait()

        cells = layers[i].reshape(R * CY, NZ)
        parts = jnp.dot(cells, matrix, preferred_element_type=F32)
        for r in range(R):
            rows = parts[r * CY : (r + 1) * CY]
            c0, c1 = by_colour(rows[:, :HALF], rows[:, HALF:], x, odd_row)
            a0[r, x, PAD : PAD + CY, :] = c0
            a1[r, x, PAD : PAD + CY, :] = c1
            (xodd if x == 0 else xeven)[r] = c1.astype(BF16)

    for i in range(2):
        copies[2 + i].wait()
        cells = edge_rows[i].reshape(R * 2 * 8, NZ)
        split_rows[i] = jnp.dot(cells, matrix, preferred_element_type=F32).reshape(R, 2, 8, NZ)
    lower = side[1] == 0
    plain = side[0] == 0
    for r in range(R):
        for x in range(CX):
            if x in OUTER:
                first = a1[r, x, PAD : PAD + 1, :]
                final = a1[r, x, PAD + CY - 1 : PAD + CY, :]
            else:
                at = x - 1
                first = jnp.where(
                    plain,
                    split_rows[0, r, at, 0:1, at * HALF : (at + 1) * HALF],
                    split_rows[0, r, 1 - at, 0:1, (1 - at) * HALF : (2 - at) * HALF],
                )
                final = jnp.where(
                    plain,
                    split_rows[1, r, at, 7:8, (1 - at) * HALF : (2 - at) * HALF],
                    split_rows[1, r, 1 - at, 7:8, at * HALF : (at + 1) * HALF],
                )
            yeven[r, x : x + 1, :] = jnp.where(lower, final, first)
            yodd[r, x : x + 1, :] = jnp.where(lower, first, final)


def run_split_outer(spins):
    return call(
        split_outer,
        [STATE] * 2 + [LAYER] * 2 + [ROWS] * 2,
        [HB],
        [VM] * 6,
        [
            pltpu.VMEM((2, R, CY, NZ), BF16),
            pltpu.VMEM((2, R, 2, 8, NZ), BF16),
            pltpu.VMEM((2, R, 2, 8, NZ), F32),
            pltpu.SemaphoreType.DMA((4,)),
        ],
    )(in_hbm(spins))


def split_field(side, buf, u0, u1, matrix, plain_row):
    @pl.loop(0, R, step=4)
    def _(first):
        cells = buf[pl.ds(first, 4)].reshape(4 * CX * CY, NZ)
        parts = jnp.dot(cells, matrix, preferred_element_type=F32) * 5.0
        for k in range(4 * CX):
            rows = parts[k * CY : (k + 1) * CY]
            r, at = first + k // CX, k % CX
            x = layer_at(side, at)
            c0, c1 = by_colour(rows[:, :HALF], rows[:, HALF:], at, plain_row)
            u0[r, x] = c0
            u1[r, x] = c1


def split_inner(betas_ref, swap_ref, spins_ref, couplings_ref, uniform_ref, a0_in, a1_in, *refs):
    side = device_side()
    a0, a1, u00, u01, u10, u11, bonds0, bonds1, table, layers, bond_buf, buf, sems = refs

    copies = [
        pltpu.make_async_copy(spins_ref.at[:, pl.ds(1, 2)], layers, sems.at[0]),
        pltpu.make_async_copy(couplings_ref, bond_buf, sems.at[1]),
        pltpu.make_async_copy(uniform_ref.at[0], buf.at[0], sems.at[2]),
        pltpu.make_async_copy(uniform_ref.at[1], buf.at[1], sems.at[3]),
    ]
    for copy in copies:
        copy.start()
    matrix = split_matrix()
    plain_row = lax.broadcasted_iota(jnp.int32, (CY, HALF), 0) % 2 == 1
    fill_table(side, betas_ref, swap_ref, table)
    copies[0].wait()

    @pl.loop(0, R, step=8)
    def _(first):
        cells = layers[pl.ds(first, 8)].reshape(16 * CY, NZ)
        parts = jnp.dot(cells, matrix, preferred_element_type=F32)
        for k in range(16):
            rows = parts[k * CY : (k + 1) * CY]
            x = layer_at(side, 1 + k % 2)
            c0, c1 = by_colour(rows[:, :HALF], rows[:, HALF:], 1 + k % 2, plain_row)
            a0[first + k // 2, x, PAD : PAD + CY, :] = c0
            a1[first + k // 2, x, PAD : PAD + CY, :] = c1

    copies[1].wait()
    flip = side[0]
    for at in range(CX):
        x = layer_at(side, at)
        halves = []
        for k in range(6):
            cells = bond_buf[k, at].astype(F32).astype(BF16)
            parts = jnp.dot(cells, matrix, preferred_element_type=F32)
            halves.append((parts[:, :HALF], parts[:, HALF:]))
        for place, k in ((flip, 0), (1 - flip, 3), (2, 1), (3, 4)):
            bonds0[place, x], bonds1[place, x] = by_colour(*halves[k], at, plain_row)
        for place, (k, m) in enumerate(((2, 5), (5, 2))):
            bonds0[4 + place, x], bonds1[4 + place, x] = by_colour(halves[k][0], halves[m][1], at, plain_row)
    copies[2].wait()
    split_field(side, buf.at[0], u00, u01, matrix, plain_row)
    copies[3].wait()
    split_field(side, buf.at[1], u10, u11, matrix, plain_row)


def run_split_inner(betas, swap, spins, couplings, uniform, a0, a1):
    return call(
        split_inner,
        [STATE] * 2 + [DRAWS] * 4 + [BONDS] * 2 + [TABLE],
        [SM] * 2 + [HB] * 3 + [VM] * 2,
        [VM] * 9,
        [
            pltpu.VMEM((R, 2, CY, NZ), BF16),
            pltpu.VMEM((6, CX, CY, NZ), jnp.int32),
            pltpu.VMEM((2, R, CX, CY, NZ), BF16),
            pltpu.SemaphoreType.DMA((4,)),
        ],
        {5: 0, 6: 1},
        limit=12,
    )(betas, swap, in_hbm(spins), in_hbm(couplings), in_hbm(uniform), a0, a1)


def put_rows(table, other, yeven, yodd):
    lower = table[UPPER : UPPER + 1, :] == 0.0
    for r in range(R):
        for x in range(CX):
            even, odd = yeven[r, x : x + 1, :], yodd[r, x : x + 1, :]
            other[r, x, PAD - 1 : PAD, :] = jnp.where(lower, odd, even)
            other[r, x, PAD + CY : PAD + CY + 1, :] = jnp.where(lower, even, odd)


def update(colour, regions, table, own, other, u_ref, bonds_ref, beyond, sent, energy):
    odd_row = odd_rows_of(table, 16)

    @pl.loop(0, R, step=UNROLL)
    def _(first):
        sums = [jnp.zeros((8, HALF), F32) for _ in range(UNROLL)]
        scales = [jnp.broadcast_to(table[pl.ds(first + i, 1), :], (16, HALF)) for i in range(UNROLL)]
        for x, y, rows in regions:
            bonds = [bonds_ref[k, x, y : y + rows, :] for k in range(6)]
            odd = odd_row[:rows]
            for i in range(UNROLL):
                r = first + i

                def near(dx, dy):
                    at = x + dx
                    if at < 0:
                        return beyond[r, y : y + rows, :].astype(F32)
                    if at >= CX:
                        return beyond[r, y : y + rows, :].astype(F32)
                    return other[r, at, PAD + y + dy : PAD + y + dy + rows, :]

                same = near(0, 0)
                below, above = pltpu.roll(same, 1, 1), pltpu.roll(same, HALF - 1, 1)
                if (colour + x) % 2 == 0:
                    beside = jnp.where(odd, above, below)
                else:
                    beside = jnp.where(odd, below, above)
                field = bonds[0] * near(1, 0) + bonds[1] * near(-1, 0)
                field = field + (bonds[2] * near(0, 1) + bonds[3] * near(0, -1))
                field = field + (bonds[4] * same + bonds[5] * beside)
                spin = own[r, x, PAD + y : PAD + y + rows, :]
                accept = jnp.exp2(jnp.minimum(spin * field * scales[i][:rows], 0.0))
                new = (spin * jnp.tanh(u_ref[r, x, y : y + rows, :] - 5.0 * accept)).astype(BF16)
                wide = new.astype(F32)
                own[r, x, PAD + y : PAD + y + rows, :] = wide
                if sent is not None and x in OUTER:
                    sent[r, y : y + rows, :] = new
                if energy is not None:
                    for part in range(0, rows, 8):
                        sums[i] = sums[i] + (wide * field)[part : part + 8]
        if energy is not None:
            for i in range(UNROLL):
                energy[first + i] = sums[i]


def rows_of(layers, start=0, stop=CY, rows=16):
    return [(x, y, rows) for x in layers for y in range(start, stop, rows)]


EDGES = rows_of(INNER, 0, 8, 8) + rows_of(INNER, CY - 8, CY, 8)
ENERGY = jax.ShapeDtypeStruct((R, 8, HALF), F32)


def sweep_first(colour, table, own_in, other_in, u, bonds, halo, yeven, yodd, own, other, sent):
    put_rows(table, other, yeven, yodd)
    update(colour, rows_of(FIRST), table, own, other, u, bonds, halo, sent, None)


def sweep_last(colour, edges, table, own_in, other_in, u, bonds, halo, own, other, sent, *rest):
    update(colour, rows_of(LAST) + (EDGES if edges else []), table, own, other, u, bonds, halo, sent, None)
    if edges:
        send_rows(table, own, *rest)


def sweep_inner(colour, edges, table, own_in, other_in, u, bonds, own, other, *rest):
    regions = rows_of(INNER, 8, CY - 8) if edges else rows_of(INNER)
    update(colour, regions, table, own, other, u, bonds, None, None, None)
    if not edges:
        send_rows(table, own, *rest)


def final_inner(table, own_in, other_in, u, bonds, yeven, yodd, own, other, energy):
    put_rows(table, other, yeven, yodd)
    update(1, rows_of(INNER), table, own, other, u, bonds, None, None, energy)


def final_last(table, own_in, other_in, u, bonds, halo, so_far, own, other, energy):
    update(1, rows_of(LAST), table, own, other, u, bonds, halo, None, energy)
    energy[...] = energy[...] + so_far[...]


def final_first(table, own_in, other_in, u, bonds, halo, so_far, own, other, sums_ref, energy):
    update(1, rows_of(FIRST), table, own, other, u, bonds, halo, None, energy)
    lines = jnp.sum(energy[...] + so_far[...], axis=1)
    totals = jnp.sum(lines, axis=1, keepdims=True)
    diagonal = lax.broadcasted_iota(jnp.int32, (R, R), 0) == lax.broadcasted_iota(jnp.int32, (R, R), 1)
    row = jnp.sum(jnp.where(diagonal, totals, 0.0), axis=0, keepdims=True)
    sums_ref[...] = jnp.broadcast_to(row[None], sums_ref.shape)


def sweep_call(kernel, more_ins, more_outs, scratch=()):
    def run(*operands):
        return call(
            kernel, [STATE] * 2 + more_outs, [VM] * (5 + more_ins), [VM] * (2 + len(more_outs)), scratch, {1: 0, 2: 1}
        )(*operands)

    return run


def mix_and_join(cell_count, table, sums_ref, a0, a1, out_ref, energies_ref, weights, buf, sems):
    total = jnp.sum(sums_ref[:, 0, :], axis=0, keepdims=True)
    energies = -total / cell_count
    energies_ref[...] = energies
    side = device_side()
    betas = table[BETAS : BETAS + 1, :R]
    drawn = table[DRAWN : DRAWN + 1, :R]
    beta_step = betas[:, : R - 1] - betas[:, 1:]
    energy_step = energies[:, : R - 1] - energies[:, 1:]
    delta = swap_gain * beta_step * energy_step
    mix = jax.nn.sigmoid((jnp.minimum(delta, 0.0) - jnp.log(drawn[:, : R - 1])) / swap_width)
    for k in range(R // 2):
        weights[k : k + 1, :] = jnp.broadcast_to(mix[:, 2 * k : 2 * k + 1], (1, HALF))
    matrix = join_matrix()
    odd_row = odd_rows(side)

    def out_copy(pair):
        at = pl.ds(pair * 2, 2)
        return pltpu.make_async_copy(buf.at[at], out_ref.at[at], sems.at[pair])

    def mix_pair(pair):
        weight = jnp.broadcast_to(weights[pl.ds(pair, 1), :], (CY, HALF))
        r = pair * 2
        cells = [[], []]
        for x in range(CX):
            new = [[], []]
            for state in (a0, a1):
                upper = state[r, x, PAD : PAD + CY, :]
                lower = state[r + 1, x, PAD : PAD + CY, :]
                moved = weight * (lower - upper)
                new[0].append(upper + moved)
                new[1].append(lower - moved)
            for i in range(2):
                even, odd = by_colour(*new[i], x, odd_row)
                cells[i].append(jnp.concatenate([even.astype(BF16), odd.astype(BF16)], axis=1))
        for i in range(2):
            joined = jnp.dot(jnp.concatenate(cells[i], axis=0), matrix, preferred_element_type=F32).astype(BF16)
            for x in range(CX):
                buf[r + i, layer_at(side, x)] = joined[x * CY : (x + 1) * CY]
        out_copy(pair).start()

    @pl.loop(0, R // 2, step=PAIRS)
    def _(first):
        for i in range(PAIRS):
            mix_pair(first + i)

    @pl.loop(0, R // 2)
    def _(pair):
        out_copy(pair).wait()


def run_mix_and_join(cell_count, table, sums, a0, a1):
    return call(
        functools.partial(mix_and_join, cell_count),
        [jax.ShapeDtypeStruct((R, CX, CY, NZ), BF16), jax.ShapeDtypeStruct((1, R), F32)],
        [VM] * 4,
        [HB, VM],
        [
            pltpu.VMEM((R // 2, HALF), F32),
            pltpu.VMEM((R, CX, CY, NZ), BF16),
            pltpu.SemaphoreType.DMA((R // 2,)),
        ],
    )(table, sums, a0, a1)


def swap_pairs(x, axis, odd):
    count = lax.axis_size(axis)
    return lax.ppermute(x, axis, [(i, (((i + odd) ^ 1) - odd) % count) for i in range(count)])


def exchange(axis, even, odd):
    near = swap_pairs(even, axis, 0)
    far = swap_pairs(odd, axis, 1)
    return [near, far]


def body(spins, couplings, betas, metro_uniform, swap_uniform):
    a0, a1, xe, xo, ye, yo = run_split_outer(spins)
    xs, ys = exchange("gx", xe, xo), exchange("gy", ye, yo)
    a0, a1, u00, u01, u10, u11, bonds0, bonds1, table = run_split_inner(
        betas, swap_uniform, spins, couplings, metro_uniform, a0, a1
    )
    states = [a0, a1]
    for step, (u, bonds) in enumerate(((u00, bonds0), (u01, bonds1), (u10, bonds0))):
        colour = step % 2
        own, other = states[colour], states[1 - colour]
        edges = step == 2
        run = sweep_call(functools.partial(sweep_first, colour), 3, [LAYER])
        own, other, xo = run(table, own, other, u, bonds, xs[1], *ys)
        run = sweep_call(functools.partial(sweep_last, colour, edges), 1, [LAYER] + ([ROWS] * 2 if edges else []))
        own, other, xe, *rows = run(table, own, other, u, bonds, xs[0])
        xs = exchange("gx", xe, xo)
        if edges:
            ys = exchange("gy", *rows)
        run = sweep_call(functools.partial(sweep_inner, colour, edges), 0, [] if edges else [ROWS] * 2)
        own, other, *rows = run(table, own, other, u, bonds)
        if not edges:
            ys = exchange("gy", *rows)
        states[colour], states[1 - colour] = own, other
    both = ("gx", "gy")
    count = lax.axis_size(both)
    a0, a1 = states
    a1, a0, energy = sweep_call(final_inner, 2, [ENERGY])(table, a1, a0, u11, bonds1, *ys)
    a1, a0, energy = sweep_call(final_last, 2, [ENERGY])(table, a1, a0, u11, bonds1, xs[0], energy)
    a1, a0, sums = sweep_call(
        final_first, 2, [pltpu.VMEM((count, 1, R), F32)], [pltpu.VMEM((R, 8, HALF), F32)]
    )(table, a1, a0, u11, bonds1, xs[1], energy)
    sums = lax.all_to_all(sums, both, 0, 0, tiled=True)
    cell_count = float(CX * CY * NZ * count)
    out, energies = run_mix_and_join(
        cell_count, table, sums, a0, a1
    )
    return out, energies[0]


def solution(mesh):
    return sharded(body, mesh)


def sharded(function, mesh):
    return jax.shard_map(
        function,
        mesh=mesh,
        in_specs=(
            P(None, "gx", "gy", None),
            P(None, "gx", "gy", None),
            P(),
            P(None, None, "gx", "gy", None),
            P(),
        ),
        out_specs=(P(None, "gx", "gy", None), P()),
        check_vma=False,
    )
```

```python
import functools
import math

import jax
import jax.numpy as jnp
from jax import lax
from jax.experimental import pallas as pl
from jax.experimental.pallas import tpu as pltpu
from jax.sharding import PartitionSpec as P


R = 16
CX, CY, NZ = 4, 64, 256
HALF = NZ // 2
PAD = 8
UNROLL = 4
PAIRS = 2
FIRST, LAST, OUTER, INNER = (0,), (CX - 1,), (0, CX - 1), (1, 2)
FLIP, UPPER, BETAS, DRAWN, TABLE_ROWS = R, R + 1, R + 2, R + 3, R + 8
LOG2E = math.log2(math.e)
F32 = jnp.float32
BF16 = jnp.bfloat16
MIB = 1024 * 1024

swap_width = 0.25
swap_gain = 64.0

VM = pl.BlockSpec(memory_space=pltpu.VMEM)
SM = pl.BlockSpec(memory_space=pltpu.SMEM)
HB = pl.BlockSpec(memory_space=pltpu.HBM)


def in_hbm(x):
    return pltpu.with_memory_space_constraint(x, pltpu.HBM)


def split_matrix(gain=1.0):
    row = lax.broadcasted_iota(jnp.int32, (NZ, NZ), 0)
    col = lax.broadcasted_iota(jnp.int32, (NZ, NZ), 1)
    wanted = jnp.where(col < HALF, 2 * col, 2 * (col - HALF) + 1)
    return jnp.where(row == wanted, gain, 0.0).astype(BF16)


def join_matrix():
    row = lax.broadcasted_iota(jnp.int32, (NZ, NZ), 0)
    col = lax.broadcasted_iota(jnp.int32, (NZ, NZ), 1)
    wanted = jnp.where(row < HALF, 2 * row, 2 * (row - HALF) + 1)
    return (col == wanted).astype(F32).astype(BF16)


def device_side():
    return lax.axis_index("gx") % 2, lax.axis_index("gy") % 2


def fill_table(side, betas_ref, swap_ref, table):
    place = lax.broadcasted_iota(jnp.int32, (1, HALF), 1)
    betas = jnp.zeros((1, HALF), F32)
    drawn = jnp.ones((1, HALF), F32)
    for r in range(R):
        table[r : r + 1, :] = jnp.full((1, HALF), betas_ref[r] * (-2.0 * LOG2E), F32)
        betas = jnp.where(place == r, betas_ref[r], betas)
    for k in range(R // 2):
        drawn = jnp.where(place == 2 * k, swap_ref[k], drawn)
    for i in range(2):
        table[R + i : R + i + 1, :] = jnp.full((1, HALF), side[i], jnp.int32).astype(F32)
    table[BETAS : BETAS + 1, :] = betas
    table[DRAWN : DRAWN + 1, :] = drawn


def odd_rows_of(table, rows):
    place = lax.broadcasted_iota(jnp.int32, (rows, HALF), 0) % 2
    return place.astype(F32) != jnp.broadcast_to(table[FLIP : FLIP + 1, :], (rows, HALF))


def odd_rows(side, rows=CY):
    return (lax.broadcasted_iota(jnp.int32, (rows, HALF), 0) + side[0]) % 2 == 1


def layer_at(side, x):
    return jnp.where(side[0] == 0, x, CX - 1 - x)


def by_colour(even, odd, x, odd_row):
    if x % 2 == 0:
        return jnp.where(odd_row, odd, even), jnp.where(odd_row, even, odd)
    return jnp.where(odd_row, even, odd), jnp.where(odd_row, odd, even)


def send_rows(table, own, yeven, yodd):
    lower = table[UPPER : UPPER + 1, :] == 0.0
    for r in range(R):
        for x in range(CX):
            first = own[r, x, PAD : PAD + 1, :]
            final = own[r, x, PAD + CY - 1 : PAD + CY, :]
            yeven[r, x : x + 1, :] = jnp.where(lower, final, first)
            yodd[r, x : x + 1, :] = jnp.where(lower, first, final)


STATE = pltpu.VMEM((R, CX, CY + 2 * PAD, HALF), F32)
DRAWS = pltpu.VMEM((R, CX, CY, HALF), F32)
BONDS = pltpu.VMEM((6, CX, CY, HALF), F32)
LAYER = jax.ShapeDtypeStruct((R, CY, HALF), BF16)
ROWS = jax.ShapeDtypeStruct((R, CX, HALF), F32)
TABLE = jax.ShapeDtypeStruct((TABLE_ROWS, HALF), F32)


def call(kernel, outs, in_specs, out_specs, scratch=(), aliases={}, limit=8, flops=10**7):
    return pl.pallas_call(
        kernel,
        out_shape=outs,
        in_specs=in_specs,
        out_specs=out_specs,
        scratch_shapes=list(scratch),
        input_output_aliases=aliases,
        compiler_params=pltpu.CompilerParams(vmem_limit_bytes=limit * MIB),
        cost_estimate=pl.CostEstimate(flops=flops, bytes_accessed=2 * MIB, transcendentals=0),
    )


def split_outer(spins_ref, a0, a1, xeven, xodd, yeven, yodd, layers, edge_rows, split_rows, sems):
    side = device_side()
    copies = []
    for i, x in enumerate(OUTER):
        copies.append(pltpu.make_async_copy(spins_ref.at[:, layer_at(side, x)], layers.at[i], sems.at[i]))
    for i, y in enumerate((0, CY - 8)):
        copies.append(
            pltpu.make_async_copy(
                spins_ref.at[:, pl.ds(1, 2), pl.ds(y, 8)], edge_rows.at[i], sems.at[2 + i]
            )
        )
    for copy in copies:
        copy.start()
    matrix = split_matrix()
    odd_row = odd_rows(side)
    for i, x in enumerate(OUTER):
        copies[i].wait()

        cells = layers[i].reshape(R * CY, NZ)
        parts = jnp.dot(cells, matrix, preferred_element_type=F32)
        for r in range(R):
            rows = parts[r * CY : (r + 1) * CY]
            c0, c1 = by_colour(rows[:, :HALF], rows[:, HALF:], x, odd_row)
            a0[r, x, PAD : PAD + CY, :] = c0
            a1[r, x, PAD : PAD + CY, :] = c1
            (xodd if x == 0 else xeven)[r] = c1.astype(BF16)

    for i in range(2):
        copies[2 + i].wait()
        cells = edge_rows[i].reshape(R * 2 * 8, NZ)
        split_rows[i] = jnp.dot(cells, matrix, preferred_element_type=F32).reshape(R, 2, 8, NZ)
    lower = side[1] == 0
    plain = side[0] == 0
    for r in range(R):
        for x in range(CX):
            if x in OUTER:
                first = a1[r, x, PAD : PAD + 1, :]
                final = a1[r, x, PAD + CY - 1 : PAD + CY, :]
            else:
                at = x - 1
                first = jnp.where(
                    plain,
                    split_rows[0, r, at, 0:1, at * HALF : (at + 1) * HALF],
                    split_rows[0, r, 1 - at, 0:1, (1 - at) * HALF : (2 - at) * HALF],
                )
                final = jnp.where(
                    plain,
                    split_rows[1, r, at, 7:8, (1 - at) * HALF : (2 - at) * HALF],
                    split_rows[1, r, 1 - at, 7:8, at * HALF : (at + 1) * HALF],
                )
            yeven[r, x : x + 1, :] = jnp.where(lower, final, first)
            yodd[r, x : x + 1, :] = jnp.where(lower, first, final)


def run_split_outer(spins):
    return call(
        split_outer,
        [STATE] * 2 + [LAYER] * 2 + [ROWS] * 2,
        [HB],
        [VM] * 6,
        [
            pltpu.VMEM((2, R, CY, NZ), BF16),
            pltpu.VMEM((2, R, 2, 8, NZ), BF16),
            pltpu.VMEM((2, R, 2, 8, NZ), F32),
            pltpu.SemaphoreType.DMA((4,)),
        ],
    )(in_hbm(spins))


def split_field(side, buf, u0, u1, matrix, plain_row):
    @pl.loop(0, R, step=4)
    def _(first):
        cells = buf[pl.ds(first, 4)].reshape(4 * CX * CY, NZ)
        parts = jnp.dot(cells, matrix, preferred_element_type=F32)
        for k in range(4 * CX):
            rows = parts[k * CY : (k + 1) * CY]
            r, at = first + k // CX, k % CX
            x = layer_at(side, at)
            c0, c1 = by_colour(rows[:, :HALF], rows[:, HALF:], at, plain_row)
            u0[r, x] = c0
            u1[r, x] = c1


def split_inner(betas_ref, swap_ref, spins_ref, couplings_ref, uniform_ref, a0_in, a1_in, *refs):
    side = device_side()
    a0, a1, u00, u01, u10, u11, bonds0, bonds1, table, layers, bond_buf, buf, sems = refs

    copies = [
        pltpu.make_async_copy(spins_ref.at[:, pl.ds(1, 2)], layers, sems.at[0]),
        pltpu.make_async_copy(couplings_ref, bond_buf, sems.at[1]),
        pltpu.make_async_copy(uniform_ref.at[0], buf.at[0], sems.at[2]),
        pltpu.make_async_copy(uniform_ref.at[1], buf.at[1], sems.at[3]),
    ]
    for copy in copies:
        copy.start()
    matrix = split_matrix()
    plain_row = lax.broadcasted_iota(jnp.int32, (CY, HALF), 0) % 2 == 1
    fill_table(side, betas_ref, swap_ref, table)
    copies[0].wait()

    @pl.loop(0, R, step=8)
    def _(first):
        cells = layers[pl.ds(first, 8)].reshape(16 * CY, NZ)
        parts = jnp.dot(cells, matrix, preferred_element_type=F32)
        for k in range(16):
            rows = parts[k * CY : (k + 1) * CY]
            x = layer_at(side, 1 + k % 2)
            c0, c1 = by_colour(rows[:, :HALF], rows[:, HALF:], 1 + k % 2, plain_row)
            a0[first + k // 2, x, PAD : PAD + CY, :] = c0
            a1[first + k // 2, x, PAD : PAD + CY, :] = c1

    copies[1].wait()
    flip = side[0]
    for at in range(CX):
        x = layer_at(side, at)
        halves = []
        for k in range(6):
            cells = bond_buf[k, at].astype(F32).astype(BF16)
            parts = jnp.dot(cells, matrix, preferred_element_type=F32)
            halves.append((parts[:, :HALF], parts[:, HALF:]))
        for place, k in ((flip, 0), (1 - flip, 3), (2, 1), (3, 4)):
            bonds0[place, x], bonds1[place, x] = by_colour(*halves[k], at, plain_row)
        for place, (k, m) in enumerate(((2, 5), (5, 2))):
            bonds0[4 + place, x], bonds1[4 + place, x] = by_colour(halves[k][0], halves[m][1], at, plain_row)
    copies[2].wait()
    matrix = split_matrix(5.0)
    split_field(side, buf.at[0], u00, u01, matrix, plain_row)
    copies[3].wait()
    split_field(side, buf.at[1], u10, u11, matrix, plain_row)


def run_split_inner(betas, swap, spins, couplings, uniform, a0, a1):
    return call(
        split_inner,
        [STATE] * 2 + [DRAWS] * 4 + [BONDS] * 2 + [TABLE],
        [SM] * 2 + [HB] * 3 + [VM] * 2,
        [VM] * 9,
        [
            pltpu.VMEM((R, 2, CY, NZ), BF16),
            pltpu.VMEM((6, CX, CY, NZ), jnp.int32),
            pltpu.VMEM((2, R, CX, CY, NZ), BF16),
            pltpu.SemaphoreType.DMA((4,)),
        ],
        {5: 0, 6: 1},
        limit=12,
    )(betas, swap, in_hbm(spins), in_hbm(couplings), in_hbm(uniform), a0, a1)


def put_rows(table, other, yeven, yodd):
    lower = table[UPPER : UPPER + 1, :] == 0.0
    for r in range(R):
        for x in range(CX):
            from_even, from_odd = yeven[r, x : x + 1, :], yodd[r, x : x + 1, :]
            other[r, x, PAD - 1 : PAD, :] = jnp.where(lower, from_odd, from_even)
            other[r, x, PAD + CY : PAD + CY + 1, :] = jnp.where(lower, from_even, from_odd)


def update(colour, regions, table, own, other, u_ref, bonds_ref, beyond, sent, energy):
    odd_row = odd_rows_of(table, 16)

    @pl.loop(0, R, step=UNROLL)
    def _(first):
        sums = [jnp.zeros((8, HALF), F32) for _ in range(UNROLL)]
        scales = [jnp.broadcast_to(table[pl.ds(first + i, 1), :], (16, HALF)) for i in range(UNROLL)]
        for x, y, rows in regions:
            bonds = [bonds_ref[k, x, y : y + rows, :] for k in range(6)]
            odd = odd_row[:rows]
            for i in range(UNROLL):
                r = first + i

                def near(dx, dy):
                    at = x + dx
                    if at < 0:
                        return beyond[r, y : y + rows, :].astype(F32)
                    if at >= CX:
                        return beyond[r, y : y + rows, :].astype(F32)
                    return other[r, at, PAD + y + dy : PAD + y + dy + rows, :]

                same = near(0, 0)
                below, above = pltpu.roll(same, 1, 1), pltpu.roll(same, HALF - 1, 1)
                if (colour + x) % 2 == 0:
                    beside = jnp.where(odd, above, below)
                else:
                    beside = jnp.where(odd, below, above)
                field = bonds[0] * near(1, 0) + bonds[1] * near(-1, 0)
                field = field + (bonds[2] * near(0, 1) + bonds[3] * near(0, -1))
                field = field + (bonds[4] * same + bonds[5] * beside)
                spin = own[r, x, PAD + y : PAD + y + rows, :]
                accept = jnp.exp2(jnp.minimum(spin * field * scales[i][:rows], 0.0))
                new = (spin * jnp.tanh(u_ref[r, x, y : y + rows, :] - 5.0 * accept)).astype(BF16)
                wide = new.astype(F32)
                own[r, x, PAD + y : PAD + y + rows, :] = wide
                if sent is not None and x in OUTER:
                    sent[r, y : y + rows, :] = new
                if energy is not None:
                    for part in range(0, rows, 8):
                        sums[i] = sums[i] + (wide * field)[part : part + 8]
        if energy is not None:
            for i in range(UNROLL):
                energy[first + i] = sums[i]


def rows_of(layers, start=0, stop=CY, rows=16):
    return [(x, y, rows) for x in layers for y in range(start, stop, rows)]


EDGES = rows_of(INNER, 0, 8, 8) + rows_of(INNER, CY - 8, CY, 8)
ENERGY = jax.ShapeDtypeStruct((R, 8, HALF), F32)


def sweep_first(colour, table, own_in, other_in, u, bonds, halo, yeven, yodd, own, other, sent):
    put_rows(table, other, yeven, yodd)
    update(colour, rows_of(FIRST), table, own, other, u, bonds, halo, sent, None)


def sweep_last(colour, table, own_in, other_in, u, bonds, halo, own, other, sent):
    update(colour, rows_of(LAST), table, own, other, u, bonds, halo, sent, None)


def sweep_edges(colour, table, own_in, other_in, u, bonds, own, other, yeven, yodd):
    update(colour, EDGES, table, own, other, u, bonds, None, None, None)
    send_rows(table, own, yeven, yodd)


def sweep_inner(colour, table, own_in, other_in, u, bonds, own, other):
    update(colour, rows_of(INNER, 8, CY - 8), table, own, other, u, bonds, None, None, None)


def final_inner(table, own_in, other_in, u, bonds, own, other, energy):
    update(1, rows_of(INNER, 8, CY - 8), table, own, other, u, bonds, None, None, energy)


def final_first(table, own_in, other_in, u, bonds, halo, yeven, yodd, so_far, own, other, energy):
    put_rows(table, other, yeven, yodd)
    update(1, rows_of(FIRST), table, own, other, u, bonds, halo, None, energy)
    energy[...] = energy[...] + so_far[...]


def final_last(table, own_in, other_in, u, bonds, halo, so_far, own, other, sums_ref, energy):
    update(1, rows_of(LAST) + EDGES, table, own, other, u, bonds, halo, None, energy)
    lines = jnp.sum(energy[...] + so_far[...], axis=1)
    totals = jnp.sum(lines, axis=1, keepdims=True)
    diagonal = lax.broadcasted_iota(jnp.int32, (R, R), 0) == lax.broadcasted_iota(jnp.int32, (R, R), 1)
    row = jnp.sum(jnp.where(diagonal, totals, 0.0), axis=0, keepdims=True)
    sums_ref[...] = jnp.broadcast_to(row[None], sums_ref.shape)


def sweep_call(kernel, more_ins, more_outs, scratch=()):
    def run(*operands):
        return call(
            kernel, [STATE] * 2 + more_outs, [VM] * (5 + more_ins), [VM] * (2 + len(more_outs)), scratch, {1: 0, 2: 1}
        )(*operands)

    return run


def mix_and_join(cell_count, table, sums_ref, a0, a1, out_ref, energies_ref, weights, buf, sems):
    total = jnp.sum(sums_ref[:, 0, :], axis=0, keepdims=True)
    energies = -total / cell_count
    energies_ref[...] = energies
    side = device_side()
    betas = table[BETAS : BETAS + 1, :R]
    drawn = table[DRAWN : DRAWN + 1, :R]
    beta_step = betas[:, : R - 1] - betas[:, 1:]
    energy_step = energies[:, : R - 1] - energies[:, 1:]
    delta = swap_gain * beta_step * energy_step
    mix = jax.nn.sigmoid((jnp.minimum(delta, 0.0) - jnp.log(drawn[:, : R - 1])) / swap_width)
    for k in range(R // 2):
        weights[k : k + 1, :] = jnp.broadcast_to(mix[:, 2 * k : 2 * k + 1], (1, HALF))
    matrix = join_matrix()
    odd_row = odd_rows(side)

    def out_copy(pair):
        at = pl.ds(pair * 2, 2)
        return pltpu.make_async_copy(buf.at[at], out_ref.at[at], sems.at[pair])

    def mix_pair(pair):
        weight = jnp.broadcast_to(weights[pl.ds(pair, 1), :], (CY, HALF))
        r = pair * 2
        cells = [[], []]
        for x in range(CX):
            new = [[], []]
            for state in (a0, a1):
                upper = state[r, x, PAD : PAD + CY, :]
                lower = state[r + 1, x, PAD : PAD + CY, :]
                moved = weight * (lower - upper)
                new[0].append(upper + moved)
                new[1].append(lower - moved)
            for i in range(2):
                even, odd = by_colour(*new[i], x, odd_row)
                cells[i].append(jnp.concatenate([even.astype(BF16), odd.astype(BF16)], axis=1))
        for i in range(2):
            joined = jnp.dot(jnp.concatenate(cells[i], axis=0), matrix, preferred_element_type=F32).astype(BF16)
            for x in range(CX):
                buf[r + i, layer_at(side, x)] = joined[x * CY : (x + 1) * CY]
        out_copy(pair).start()

    @pl.loop(0, R // 2, step=PAIRS)
    def _(first):
        for i in range(PAIRS):
            mix_pair(first + i)

    @pl.loop(0, R // 2)
    def _(pair):
        out_copy(pair).wait()


def run_mix_and_join(cell_count, table, sums, a0, a1):
    return call(
        functools.partial(mix_and_join, cell_count),
        [jax.ShapeDtypeStruct((R, CX, CY, NZ), BF16), jax.ShapeDtypeStruct((1, R), F32)],
        [VM] * 4,
        [HB, VM],
        [
            pltpu.VMEM((R // 2, HALF), F32),
            pltpu.VMEM((R, CX, CY, NZ), BF16),
            pltpu.SemaphoreType.DMA((R // 2,)),
        ],
    )(table, sums, a0, a1)


def swap_pairs(x, axis, odd):
    count = lax.axis_size(axis)
    return lax.ppermute(x, axis, [(i, (((i + odd) ^ 1) - odd) % count) for i in range(count)])


def exchange_layers(first, last):
    first = swap_pairs(first, "gx", 1)
    last = swap_pairs(last, "gx", 0)
    return first, last


def exchange_rows(even, odd):
    return swap_pairs(even, "gy", 0), swap_pairs(odd, "gy", 1)


def body(spins, couplings, betas, metro_uniform, swap_uniform):
    a0, a1, xe, xo, ye, yo = run_split_outer(spins)
    xs, ys = exchange_layers(xo, xe), exchange_rows(ye, yo)
    a0, a1, u00, u01, u10, u11, bonds0, bonds1, table = run_split_inner(
        betas, swap_uniform, spins, couplings, metro_uniform, a0, a1
    )
    states = [a0, a1]
    for step, (u, bonds) in enumerate(((u00, bonds0), (u01, bonds1), (u10, bonds0))):
        colour = step % 2
        own, other = states[colour], states[1 - colour]
        run = sweep_call(functools.partial(sweep_first, colour), 3, [LAYER])
        own, other, xo = run(table, own, other, u, bonds, xs[0], *ys)
        run = sweep_call(functools.partial(sweep_last, colour), 1, [LAYER])
        own, other, xe = run(table, own, other, u, bonds, xs[1])
        xs = exchange_layers(xo, xe)
        run = sweep_call(functools.partial(sweep_edges, colour), 0, [ROWS] * 2)
        own, other, *rows = run(table, own, other, u, bonds)
        ys = exchange_rows(*rows)
        run = sweep_call(functools.partial(sweep_inner, colour), 0, [])
        own, other = run(table, own, other, u, bonds)
        states[colour], states[1 - colour] = own, other
    both = ("gx", "gy")
    count = lax.axis_size(both)
    a0, a1 = states
    a1, a0, energy = sweep_call(final_inner, 0, [ENERGY])(table, a1, a0, u11, bonds1)
    a1, a0, energy = sweep_call(final_first, 4, [ENERGY])(table, a1, a0, u11, bonds1, xs[0], *ys, energy)
    a1, a0, sums = sweep_call(
        final_last, 2, [pltpu.VMEM((count, 1, R), F32)], [pltpu.VMEM((R, 8, HALF), F32)]
    )(table, a1, a0, u11, bonds1, xs[1], energy)
    sums = lax.all_to_all(sums, both, 0, 0, tiled=True)
    cell_count = float(CX * CY * NZ * count)
    out, energies = run_mix_and_join(
        cell_count, table, sums, a0, a1
    )
    return out, energies[0]


def solution(mesh):
    return sharded(body, mesh)


def sharded(function, mesh):
    return jax.shard_map(
        function,
        mesh=mesh,
        in_specs=(
            P(None, "gx", "gy", None),
            P(None, "gx", "gy", None),
            P(),
            P(None, None, "gx", "gy", None),
            P(),
        ),
        out_specs=(P(None, "gx", "gy", None), P()),
        check_vma=False,
    )
```

```python
import functools
import math

import jax
import jax.numpy as jnp
from jax import lax
from jax.experimental import pallas as pl
from jax.experimental.pallas import tpu as pltpu
from jax.sharding import PartitionSpec as P


R = 16
CX, CY, NZ = 4, 64, 256
HALF = NZ // 2
PAD = 8
UNROLL = 4
PAIRS = 2
FIRST, LAST, OUTER, INNER = (0,), (CX - 1,), (0, CX - 1), (1, 2)
FLIP, UPPER, BETAS, DRAWN, TABLE_ROWS = R, R + 1, R + 2, R + 3, R + 8
LOG2E = math.log2(math.e)
F32 = jnp.float32
BF16 = jnp.bfloat16
MIB = 1024 * 1024

swap_width = 0.25
swap_gain = 64.0

VM = pl.BlockSpec(memory_space=pltpu.VMEM)
SM = pl.BlockSpec(memory_space=pltpu.SMEM)
HB = pl.BlockSpec(memory_space=pltpu.HBM)


def in_hbm(x):
    return pltpu.with_memory_space_constraint(x, pltpu.HBM)


def split_matrix(gain=1.0):
    row = lax.broadcasted_iota(jnp.int32, (NZ, NZ), 0)
    col = lax.broadcasted_iota(jnp.int32, (NZ, NZ), 1)
    wanted = jnp.where(col < HALF, 2 * col, 2 * (col - HALF) + 1)
    return jnp.where(row == wanted, gain, 0.0).astype(BF16)


def join_matrix():
    row = lax.broadcasted_iota(jnp.int32, (NZ, NZ), 0)
    col = lax.broadcasted_iota(jnp.int32, (NZ, NZ), 1)
    wanted = jnp.where(row < HALF, 2 * row, 2 * (row - HALF) + 1)
    return (col == wanted).astype(F32).astype(BF16)


def device_side():
    return lax.axis_index("gx") % 2, lax.axis_index("gy") % 2


def fill_table(side, betas_ref, swap_ref, table):
    place = lax.broadcasted_iota(jnp.int32, (1, HALF), 1)
    betas = jnp.zeros((1, HALF), F32)
    drawn = jnp.ones((1, HALF), F32)
    for r in range(R):
        table[r : r + 1, :] = jnp.full((1, HALF), betas_ref[r] * (-2.0 * LOG2E), F32)
        betas = jnp.where(place == r, betas_ref[r], betas)
    for k in range(R // 2):
        drawn = jnp.where(place == 2 * k, swap_ref[k], drawn)
    for i in range(2):
        table[R + i : R + i + 1, :] = jnp.full((1, HALF), side[i], jnp.int32).astype(F32)
    table[BETAS : BETAS + 1, :] = betas
    table[DRAWN : DRAWN + 1, :] = drawn


def odd_rows_of(table, rows):
    place = lax.broadcasted_iota(jnp.int32, (rows, HALF), 0) % 2
    return place.astype(F32) != jnp.broadcast_to(table[FLIP : FLIP + 1, :], (rows, HALF))


def odd_rows(side, rows=CY):
    return (lax.broadcasted_iota(jnp.int32, (rows, HALF), 0) + side[0]) % 2 == 1


def layer_at(side, x):
    return jnp.where(side[0] == 0, x, CX - 1 - x)


def by_colour(even, odd, x, odd_row):
    if x % 2 == 0:
        return jnp.where(odd_row, odd, even), jnp.where(odd_row, even, odd)
    return jnp.where(odd_row, even, odd), jnp.where(odd_row, odd, even)


def send_rows(table, own, yeven, yodd):
    lower = table[UPPER : UPPER + 1, :] == 0.0
    for r in range(R):
        for x in range(CX):
            first = own[r, x, PAD : PAD + 1, :]
            final = own[r, x, PAD + CY - 1 : PAD + CY, :]
            yeven[r, x : x + 1, :] = jnp.where(lower, final, first)
            yodd[r, x : x + 1, :] = jnp.where(lower, first, final)


STATE = pltpu.VMEM((R, CX, CY + 2 * PAD, HALF), F32)
DRAWS = pltpu.VMEM((R, CX, CY, HALF), F32)
BONDS = pltpu.VMEM((6, CX, CY, HALF), F32)
LAYER = jax.ShapeDtypeStruct((R, CY, HALF), BF16)
ROWS = jax.ShapeDtypeStruct((R, CX, HALF), F32)
TABLE = jax.ShapeDtypeStruct((TABLE_ROWS, HALF), F32)


def call(kernel, outs, in_specs, out_specs, scratch=(), aliases={}, limit=8, flops=10**7):
    return pl.pallas_call(
        kernel,
        out_shape=outs,
        in_specs=in_specs,
        out_specs=out_specs,
        scratch_shapes=list(scratch),
        input_output_aliases=aliases,
        compiler_params=pltpu.CompilerParams(vmem_limit_bytes=limit * MIB),
        cost_estimate=pl.CostEstimate(flops=flops, bytes_accessed=2 * MIB, transcendentals=0),
    )


def split_outer(spins_ref, a0, a1, xeven, xodd, yeven, yodd, layers, edge_rows, split_rows, sems):
    side = device_side()
    copies = []
    for i, x in enumerate(OUTER):
        copies.append(pltpu.make_async_copy(spins_ref.at[:, layer_at(side, x)], layers.at[i], sems.at[i]))
    for i, y in enumerate((0, CY - 8)):
        copies.append(
            pltpu.make_async_copy(
                spins_ref.at[:, pl.ds(1, 2), pl.ds(y, 8)], edge_rows.at[i], sems.at[2 + i]
            )
        )
    for copy in copies:
        copy.start()
    matrix = split_matrix()
    odd_row = odd_rows(side)
    for i, x in enumerate(OUTER):
        copies[i].wait()

        cells = layers[i].reshape(R * CY, NZ)
        parts = jnp.dot(cells, matrix, preferred_element_type=F32)
        for r in range(R):
            rows = parts[r * CY : (r + 1) * CY]
            c0, c1 = by_colour(rows[:, :HALF], rows[:, HALF:], x, odd_row)
            a0[r, x, PAD : PAD + CY, :] = c0
            a1[r, x, PAD : PAD + CY, :] = c1
            (xodd if x == 0 else xeven)[r] = c1.astype(BF16)

    for i in range(2):
        copies[2 + i].wait()
        cells = edge_rows[i].reshape(R * 2 * 8, NZ)
        split_rows[i] = jnp.dot(cells, matrix, preferred_element_type=F32).reshape(R, 2, 8, NZ)
    lower = side[1] == 0
    plain = side[0] == 0
    for r in range(R):
        for x in range(CX):
            if x in OUTER:
                first = a1[r, x, PAD : PAD + 1, :]
                final = a1[r, x, PAD + CY - 1 : PAD + CY, :]
            else:
                at = x - 1
                first = jnp.where(
                    plain,
                    split_rows[0, r, at, 0:1, at * HALF : (at + 1) * HALF],
                    split_rows[0, r, 1 - at, 0:1, (1 - at) * HALF : (2 - at) * HALF],
                )
                final = jnp.where(
                    plain,
                    split_rows[1, r, at, 7:8, (1 - at) * HALF : (2 - at) * HALF],
                    split_rows[1, r, 1 - at, 7:8, at * HALF : (at + 1) * HALF],
                )
            yeven[r, x : x + 1, :] = jnp.where(lower, final, first)
            yodd[r, x : x + 1, :] = jnp.where(lower, first, final)


def run_split_outer(spins):
    return call(
        split_outer,
        [STATE] * 2 + [LAYER] * 2 + [ROWS] * 2,
        [HB],
        [VM] * 6,
        [
            pltpu.VMEM((2, R, CY, NZ), BF16),
            pltpu.VMEM((2, R, 2, 8, NZ), BF16),
            pltpu.VMEM((2, R, 2, 8, NZ), F32),
            pltpu.SemaphoreType.DMA((4,)),
        ],
    )(in_hbm(spins))


def split_field(side, buf, u0, u1, matrix, plain_row):
    @pl.loop(0, R, step=4)
    def _(first):
        cells = buf[pl.ds(first, 4)].reshape(4 * CX * CY, NZ)
        parts = jnp.dot(cells, matrix, preferred_element_type=F32)
        for k in range(4 * CX):
            rows = parts[k * CY : (k + 1) * CY]
            r, at = first + k // CX, k % CX
            x = layer_at(side, at)
            c0, c1 = by_colour(rows[:, :HALF], rows[:, HALF:], at, plain_row)
            u0[r, x] = c0
            u1[r, x] = c1


def split_inner(betas_ref, swap_ref, spins_ref, couplings_ref, uniform_ref, a0_in, a1_in, *refs):
    side = device_side()
    a0, a1, u00, u01, u10, u11, bonds0, bonds1, table, layers, bond_buf, buf, sems = refs

    copies = [
        pltpu.make_async_copy(spins_ref.at[:, pl.ds(1, 2)], layers, sems.at[0]),
        pltpu.make_async_copy(couplings_ref, bond_buf, sems.at[1]),
        pltpu.make_async_copy(uniform_ref.at[0], buf.at[0], sems.at[2]),
        pltpu.make_async_copy(uniform_ref.at[1], buf.at[1], sems.at[3]),
    ]
    for copy in copies:
        copy.start()
    matrix = split_matrix()
    plain_row = lax.broadcasted_iota(jnp.int32, (CY, HALF), 0) % 2 == 1
    fill_table(side, betas_ref, swap_ref, table)
    copies[0].wait()

    @pl.loop(0, R, step=8)
    def _(first):
        cells = layers[pl.ds(first, 8)].reshape(16 * CY, NZ)
        parts = jnp.dot(cells, matrix, preferred_element_type=F32)
        for k in range(16):
            rows = parts[k * CY : (k + 1) * CY]
            x = layer_at(side, 1 + k % 2)
            c0, c1 = by_colour(rows[:, :HALF], rows[:, HALF:], 1 + k % 2, plain_row)
            a0[first + k // 2, x, PAD : PAD + CY, :] = c0
            a1[first + k // 2, x, PAD : PAD + CY, :] = c1

    copies[1].wait()
    flip = side[0]
    for at in range(CX):
        x = layer_at(side, at)
        halves = []
        for k in range(6):
            cells = bond_buf[k, at].astype(F32).astype(BF16)
            parts = jnp.dot(cells, matrix, preferred_element_type=F32)
            halves.append((parts[:, :HALF], parts[:, HALF:]))
        for place, k in ((flip, 0), (1 - flip, 3), (2, 1), (3, 4)):
            bonds0[place, x], bonds1[place, x] = by_colour(*halves[k], at, plain_row)
        for place, (k, m) in enumerate(((2, 5), (5, 2))):
            bonds0[4 + place, x], bonds1[4 + place, x] = by_colour(halves[k][0], halves[m][1], at, plain_row)
    copies[2].wait()
    matrix = split_matrix(5.0)
    split_field(side, buf.at[0], u00, u01, matrix, plain_row)
    copies[3].wait()
    split_field(side, buf.at[1], u10, u11, matrix, plain_row)


def run_split_inner(betas, swap, spins, couplings, uniform, a0, a1):
    return call(
        split_inner,
        [STATE] * 2 + [DRAWS] * 4 + [BONDS] * 2 + [TABLE],
        [SM] * 2 + [HB] * 3 + [VM] * 2,
        [VM] * 9,
        [
            pltpu.VMEM((R, 2, CY, NZ), BF16),
            pltpu.VMEM((6, CX, CY, NZ), jnp.int32),
            pltpu.VMEM((2, R, CX, CY, NZ), BF16),
            pltpu.SemaphoreType.DMA((4,)),
        ],
        {5: 0, 6: 1},
        limit=12,
    )(betas, swap, in_hbm(spins), in_hbm(couplings), in_hbm(uniform), a0, a1)


def put_rows(table, other, yeven, yodd):
    lower = table[UPPER : UPPER + 1, :] == 0.0
    for r in range(R):
        for x in range(CX):
            from_even, from_odd = yeven[r, x : x + 1, :], yodd[r, x : x + 1, :]
            other[r, x, PAD - 1 : PAD, :] = jnp.where(lower, from_odd, from_even)
            other[r, x, PAD + CY : PAD + CY + 1, :] = jnp.where(lower, from_even, from_odd)


def update(colour, regions, table, own, other, u_ref, bonds_ref, beyond, sent, energy):
    odd_row = odd_rows_of(table, 16)

    @pl.loop(0, R, step=UNROLL)
    def _(first):
        sums = [jnp.zeros((8, HALF), F32) for _ in range(UNROLL)]
        scales = [jnp.broadcast_to(table[pl.ds(first + i, 1), :], (16, HALF)) for i in range(UNROLL)]
        for x, y, rows in regions:
            bonds = [bonds_ref[k, x, y : y + rows, :] for k in range(6)]
            odd = odd_row[:rows]
            for i in range(UNROLL):
                r = first + i

                def near(dx, dy):
                    at = x + dx
                    if at < 0:
                        return beyond[r, y : y + rows, :].astype(F32)
                    if at >= CX:
                        return beyond[r, y : y + rows, :].astype(F32)
                    return other[r, at, PAD + y + dy : PAD + y + dy + rows, :]

                same = near(0, 0)
                below, above = pltpu.roll(same, 1, 1), pltpu.roll(same, HALF - 1, 1)
                if (colour + x) % 2 == 0:
                    beside = jnp.where(odd, above, below)
                else:
                    beside = jnp.where(odd, below, above)
                field = bonds[0] * near(1, 0) + bonds[1] * near(-1, 0)
                field = field + (bonds[2] * near(0, 1) + bonds[3] * near(0, -1))
                field = field + (bonds[4] * same + bonds[5] * beside)
                spin = own[r, x, PAD + y : PAD + y + rows, :]
                accept = jnp.exp2(jnp.minimum(spin * field * scales[i][:rows], 0.0))
                new = (spin * jnp.tanh(u_ref[r, x, y : y + rows, :] - 5.0 * accept)).astype(BF16)
                wide = new.astype(F32)
                own[r, x, PAD + y : PAD + y + rows, :] = wide
                if sent is not None and x in OUTER:
                    sent[r, y : y + rows, :] = new
                if energy is not None:
                    for part in range(0, rows, 8):
                        sums[i] = sums[i] + (wide * field)[part : part + 8]
        if energy is not None:
            for i in range(UNROLL):
                energy[first + i] = sums[i]


def rows_of(layers, start=0, stop=CY, rows=16):
    return [(x, y, rows) for x in layers for y in range(start, stop, rows)]


EDGES = rows_of(INNER, 0, 8, 8) + rows_of(INNER, CY - 8, CY, 8)
ENERGY = jax.ShapeDtypeStruct((R, 8, HALF), F32)


def sweep_first(colour, table, own_in, other_in, u, bonds, halo, yeven, yodd, own, other, sent):
    put_rows(table, other, yeven, yodd)
    update(colour, rows_of(FIRST), table, own, other, u, bonds, halo, sent, None)


def sweep_last(colour, table, own_in, other_in, u, bonds, halo, own, other, sent):
    update(colour, rows_of(LAST), table, own, other, u, bonds, halo, sent, None)


def sweep_edges(colour, table, own_in, other_in, u, bonds, own, other, yeven, yodd):
    update(colour, EDGES, table, own, other, u, bonds, None, None, None)
    send_rows(table, own, yeven, yodd)


def sweep_inner(colour, table, own_in, other_in, u, bonds, own, other):
    update(colour, rows_of(INNER, 8, CY - 8), table, own, other, u, bonds, None, None, None)


def final_inner(table, own_in, other_in, u, bonds, own, other, energy):
    update(1, rows_of(INNER, 8, CY - 8), table, own, other, u, bonds, None, None, energy)


def final_first(table, own_in, other_in, u, bonds, halo, yeven, yodd, so_far, own, other, energy):
    put_rows(table, other, yeven, yodd)
    update(1, rows_of(FIRST), table, own, other, u, bonds, halo, None, energy)
    energy[...] = energy[...] + so_far[...]


def final_last(table, own_in, other_in, u, bonds, halo, so_far, own, other, sums_ref, energy):
    update(1, rows_of(LAST) + EDGES, table, own, other, u, bonds, halo, None, energy)
    lines = jnp.sum(energy[...] + so_far[...], axis=1)
    totals = jnp.sum(lines, axis=1, keepdims=True)
    diagonal = lax.broadcasted_iota(jnp.int32, (R, R), 0) == lax.broadcasted_iota(jnp.int32, (R, R), 1)
    row = jnp.sum(jnp.where(diagonal, totals, 0.0), axis=0, keepdims=True)
    sums_ref[...] = jnp.broadcast_to(row[None], sums_ref.shape)


def sweep_call(kernel, more_ins, more_outs, scratch=()):
    def run(*operands):
        return call(
            kernel,
            [STATE] * 2 + more_outs,
            [VM] * (5 + more_ins),
            [VM] * (2 + len(more_outs)),
            scratch,
            {1: 0, 2: 1},
        )(*operands)

    return run


def mix_and_join(cell_count, table, sums_ref, a0, a1, out_ref, energies_ref, weights, buf, sems):
    total = jnp.sum(sums_ref[:, 0, :], axis=0, keepdims=True)
    energies = -total / cell_count
    energies_ref[...] = energies
    side = device_side()
    betas = table[BETAS : BETAS + 1, :R]
    drawn = table[DRAWN : DRAWN + 1, :R]
    beta_step = betas[:, : R - 1] - betas[:, 1:]
    energy_step = energies[:, : R - 1] - energies[:, 1:]
    delta = swap_gain * beta_step * energy_step
    mix = jax.nn.sigmoid((jnp.minimum(delta, 0.0) - jnp.log(drawn[:, : R - 1])) / swap_width)
    for k in range(R // 2):
        weights[k : k + 1, :] = jnp.broadcast_to(mix[:, 2 * k : 2 * k + 1], (1, HALF))
    matrix = join_matrix()
    odd_row = odd_rows(side)

    def out_copy(pair):
        at = pl.ds(pair * 2, 2)
        return pltpu.make_async_copy(buf.at[at], out_ref.at[at], sems.at[pair])

    def mix_pair(pair):
        weight = jnp.broadcast_to(weights[pl.ds(pair, 1), :], (CY, HALF))
        r = pair * 2
        cells = [[], []]
        for x in range(CX):
            new = [[], []]
            for state in (a0, a1):
                upper = state[r, x, PAD : PAD + CY, :]
                lower = state[r + 1, x, PAD : PAD + CY, :]
                moved = weight * (lower - upper)
                new[0].append(upper + moved)
                new[1].append(lower - moved)
            for i in range(2):
                even, odd = by_colour(*new[i], x, odd_row)
                cells[i].append(jnp.concatenate([even.astype(BF16), odd.astype(BF16)], axis=1))
        for i in range(2):
            joined = jnp.dot(jnp.concatenate(cells[i], axis=0), matrix, preferred_element_type=F32).astype(BF16)
            for x in range(CX):
                buf[r + i, layer_at(side, x)] = joined[x * CY : (x + 1) * CY]
        out_copy(pair).start()

    @pl.loop(0, R // 2, step=PAIRS)
    def _(first):
        for i in range(PAIRS):
            mix_pair(first + i)

    @pl.loop(0, R // 2)
    def _(pair):
        out_copy(pair).wait()


def run_mix_and_join(cell_count, table, sums, a0, a1):
    return call(
        functools.partial(mix_and_join, cell_count),
        [jax.ShapeDtypeStruct((R, CX, CY, NZ), BF16), jax.ShapeDtypeStruct((1, R), F32)],
        [VM] * 4,
        [HB, VM],
        [
            pltpu.VMEM((R // 2, HALF), F32),
            pltpu.VMEM((R, CX, CY, NZ), BF16),
            pltpu.SemaphoreType.DMA((R // 2,)),
        ],
    )(table, sums, a0, a1)


def swap_pairs(x, axis, odd):
    count = lax.axis_size(axis)
    return lax.ppermute(x, axis, [(i, (((i + odd) ^ 1) - odd) % count) for i in range(count)])


def exchange_layers(first, last):
    first = swap_pairs(first, "gx", 1)
    last = swap_pairs(last, "gx", 0)
    return first, last


def exchange_rows(even, odd):
    even = swap_pairs(even, "gy", 0)
    odd = swap_pairs(odd, "gy", 1)
    return even, odd


def body(spins, couplings, betas, metro_uniform, swap_uniform):
    a0, a1, xe, xo, ye, yo = run_split_outer(spins)
    xs, ys = exchange_layers(xo, xe), exchange_rows(ye, yo)
    a0, a1, u00, u01, u10, u11, bonds0, bonds1, table = run_split_inner(
        betas, swap_uniform, spins, couplings, metro_uniform, a0, a1
    )
    states = [a0, a1]
    for step, (u, bonds) in enumerate(((u00, bonds0), (u01, bonds1), (u10, bonds0))):
        colour = step % 2
        own, other = states[colour], states[1 - colour]
        run = sweep_call(functools.partial(sweep_first, colour), 3, [LAYER])
        own, other, xo = run(table, own, other, u, bonds, xs[0], *ys)
        run = sweep_call(functools.partial(sweep_last, colour), 1, [LAYER])
        own, other, xe = run(table, own, other, u, bonds, xs[1])
        xs = exchange_layers(xo, xe)
        run = sweep_call(functools.partial(sweep_edges, colour), 0, [ROWS] * 2)
        own, other, *rows = run(table, own, other, u, bonds)
        ys = exchange_rows(*rows)
        run = sweep_call(functools.partial(sweep_inner, colour), 0, [])
        own, other = run(table, own, other, u, bonds)
        states[colour], states[1 - colour] = own, other
    both = ("gx", "gy")
    count = lax.axis_size(both)
    a0, a1 = states
    a1, a0, energy = sweep_call(final_inner, 0, [ENERGY])(table, a1, a0, u11, bonds1)
    a1, a0, energy = sweep_call(final_first, 4, [ENERGY])(table, a1, a0, u11, bonds1, xs[0], *ys, energy)
    a1, a0, sums = sweep_call(
        final_last, 2, [pltpu.VMEM((count, 1, R), F32)], [pltpu.VMEM((R, 8, HALF), F32)]
    )(table, a1, a0, u11, bonds1, xs[1], energy)
    sums = lax.all_to_all(sums, both, 0, 0, tiled=True)
    cell_count = float(CX * CY * NZ * count)
    out, energies = run_mix_and_join(
        cell_count, table, sums, a0, a1
    )
    return out, energies[0]


def solution(mesh):
    return sharded(body, mesh)


def sharded(function, mesh):
    return jax.shard_map(
        function,
        mesh=mesh,
        in_specs=(
            P(None, "gx", "gy", None),
            P(None, "gx", "gy", None),
            P(),
            P(None, None, "gx", "gy", None),
            P(),
        ),
        out_specs=(P(None, "gx", "gy", None), P()),
        check_vma=False,
    )
```
